64 devices in a mesh: dp: 4 (over x, y), tp: 16 (over z, core).
Axes of the slice: x: 2, y: 2, z: 8, core: 2. Of those that a mesh axis runs over, the one named last changes fastest.
The devices are a block of a 4x4x8 slice.
Arguments:
- hidden: bfloat16 [4, 2048, 2560], P('dp'), parts along dimension 0
- grad_out: bfloat16 [4, 2048, 2560], P('dp'), parts along dimension 0
- norm_gain: bfloat16 [2560], replicated
- w_query: bfloat16 [2560, 4096], P(None, 'tp')
- w_key: bfloat16 [2560, 1024], replicated
- w_value: bfloat16 [2560, 1024], replicated
- w_out: bfloat16 [4096, 2560], P('tp')
Outputs:
- output 1: bfloat16 [4, 2048, 2560], P('dp'), parts along dimension 0
- output 2: bfloat16 [4, 2048, 2560], P('dp'), parts along dimension 0
- output 3: float32 [10240], P('dp'), parts along dimension 0
- output 4: float32 [10240, 4096], P('dp', 'tp'), parts along dimension 0
- output 5: float32 [10240, 2048], P('dp', 'tp'), parts along dimension 0
- output 6: float32 [10240, 2048], P('dp', 'tp'), parts along dimension 0
- output 7: float32 [16384, 2560], P(('dp', 'tp')), parts along dimension 0
There are 4 independent parts. The reference program is written for one: setup_inputs(seed, part) draws one part's arguments, and reference() takes and returns one part's arrays. A program takes and returns all parts, laid end to end along the dimension named above; an argument that names none is the same for every part.
All inputs are finite; a program needn't handle non-finite values.
Results may differ from the reference program's by a relative error of at most 0.0098541.
Values sent between devices are 32-bit elements.
A program may use at most 768 MiB of HBM per device.

```python
import math
import jax
import jax.numpy as jnp
from jax import lax

BATCH_SIZE = 1
SEQ_LEN = 2048
D_MODEL = 2560
Q_HEADS = 32
KV_HEADS = 8
HEAD_DIM = 128
TP_SIZE = 16
NORM_EPS = 1.0e-5
ROPE_BASE = 10000.0
MASK_VALUE = -1.0e30


def setup_inputs(seed: int = 0, part: int = 0) -> dict:
    root_key = jax.random.key(seed)
    shared_key, local_key = jax.random.split(root_key)
    part_key = jax.random.fold_in(local_key, part)
    key_hidden, key_grad = jax.random.split(part_key)
    key_gain, key_query, key_key, key_value, key_out = jax.random.split(shared_key, 5)
    inner_width = Q_HEADS * HEAD_DIM
    kv_width = KV_HEADS * HEAD_DIM
    score_gain = math.sqrt(0.5 * math.log(SEQ_LEN))
    act_shape = (BATCH_SIZE, SEQ_LEN, D_MODEL)
    hidden = jax.random.normal(key_hidden, act_shape, jnp.float32)
    grad_out = jax.random.normal(key_grad, act_shape, jnp.float32)
    norm_gain = 1.0 + 0.3 * jax.random.normal(key_gain, (D_MODEL,), jnp.float32)
    w_query = jax.random.normal(key_query, (D_MODEL, inner_width), jnp.float32) * (score_gain / math.sqrt(D_MODEL))
    w_key = jax.random.normal(key_key, (D_MODEL, kv_width), jnp.float32) / math.sqrt(D_MODEL)
    w_value = jax.random.normal(key_value, (D_MODEL, kv_width), jnp.float32) / math.sqrt(D_MODEL)
    w_out = jax.random.normal(key_out, (inner_width, D_MODEL), jnp.float32) * (3.0 / math.sqrt(inner_width))
    return {
        'hidden': hidden.astype(jnp.bfloat16),
        'grad_out': grad_out.astype(jnp.bfloat16),
        'norm_gain': norm_gain.astype(jnp.bfloat16),
        'w_query': w_query.astype(jnp.bfloat16),
        'w_key': w_key.astype(jnp.bfloat16),
        'w_value': w_value.astype(jnp.bfloat16),
        'w_out': w_out.astype(jnp.bfloat16),
    }


def to_bf16(tensor):
    return tensor + lax.stop_gradient(tensor.astype(jnp.bfloat16).astype(tensor.dtype) - tensor)


def rope_tables():
    positions = jnp.arange(SEQ_LEN, dtype=jnp.float32)
    inv_freq = ROPE_BASE ** (-jnp.arange(0, HEAD_DIM, 2, dtype=jnp.float32) / HEAD_DIM)
    angles = positions[:, None] * inv_freq[None, :]
    return jnp.cos(angles), jnp.sin(angles)


def rotate_pairs(tensor, cos_t, sin_t):
    pair_view = tensor.reshape(tensor.shape[:-1] + (HEAD_DIM // 2, 2))
    even_part = pair_view[..., 0]
    odd_part = pair_view[..., 1]
    cos_b = cos_t[:, None, :]
    sin_b = sin_t[:, None, :]
    rotated = jnp.stack([even_part * cos_b - odd_part * sin_b, even_part * sin_b + odd_part * cos_b], axis=-1)
    return rotated.reshape(tensor.shape)


def group_attention(blocks):
    q_block, k_block, v_block = blocks
    scores = jnp.einsum('bqjh,bkh->bjqk', q_block, k_block) / math.sqrt(HEAD_DIM)
    causal = jnp.arange(SEQ_LEN)[:, None] >= jnp.arange(SEQ_LEN)[None, :]
    scores = jnp.where(causal, scores, MASK_VALUE)
    attn_probs = to_bf16(jax.nn.softmax(scores, axis=-1))
    return to_bf16(jnp.einsum('bjqk,bkh->bqjh', attn_probs, v_block))


def forward(hidden, norm_gain, w_query, w_key, w_value, w_out):
    heads_per_kv = Q_HEADS // KV_HEADS
    mean_sq = jnp.mean(hidden * hidden, axis=-1, keepdims=True)
    normed = to_bf16(hidden * lax.rsqrt(mean_sq + NORM_EPS) * norm_gain)
    cos_t, sin_t = rope_tables()
    q_proj = jnp.einsum('bsd,de->bse', normed, w_query).reshape(BATCH_SIZE, SEQ_LEN, Q_HEADS, HEAD_DIM)
    k_proj = jnp.einsum('bsd,de->bse', normed, w_key).reshape(BATCH_SIZE, SEQ_LEN, KV_HEADS, HEAD_DIM)
    v_proj = jnp.einsum('bsd,de->bse', normed, w_value).reshape(BATCH_SIZE, SEQ_LEN, KV_HEADS, HEAD_DIM)
    q_rot = to_bf16(rotate_pairs(q_proj, cos_t, sin_t)).reshape(BATCH_SIZE, SEQ_LEN, KV_HEADS, heads_per_kv, HEAD_DIM)
    k_rot = to_bf16(rotate_pairs(k_proj, cos_t, sin_t))
    v_heads = to_bf16(v_proj)
    attn_heads = lax.map(jax.checkpoint(group_attention), (jnp.moveaxis(q_rot, 2, 0), jnp.moveaxis(k_rot, 2, 0), jnp.moveaxis(v_heads, 2, 0)))
    attn_flat = jnp.moveaxis(attn_heads, 0, 2).reshape(BATCH_SIZE, SEQ_LEN, Q_HEADS * HEAD_DIM)
    attn_sum = jnp.einsum('bse,ed->bsd', attn_flat, w_out)
    return to_bf16(hidden + attn_sum)


def reference(hidden, grad_out, norm_gain, w_query, w_key, w_value, w_out):
    block_out, pullback = jax.vjp(forward, hidden.astype(jnp.float32), norm_gain.astype(jnp.float32), w_query.astype(jnp.float32), w_key.astype(jnp.float32), w_value.astype(jnp.float32), w_out.astype(jnp.float32))
    grad_hidden, grad_gain, grad_w_query, grad_w_key, grad_w_value, grad_w_out = pullback(grad_out.astype(jnp.float32))
    sharers = TP_SIZE // KV_HEADS
    grad_w_key_rep = jnp.repeat(grad_w_key.reshape(D_MODEL, KV_HEADS, HEAD_DIM), sharers, axis=1).reshape(D_MODEL, TP_SIZE * HEAD_DIM)
    grad_w_value_rep = jnp.repeat(grad_w_value.reshape(D_MODEL, KV_HEADS, HEAD_DIM), sharers, axis=1).reshape(D_MODEL, TP_SIZE * HEAD_DIM)
    return (block_out.astype(jnp.bfloat16), grad_hidden.astype(jnp.bfloat16), grad_gain.astype(jnp.float32), grad_w_query.astype(jnp.float32), grad_w_key_rep.astype(jnp.float32), grad_w_value_rep.astype(jnp.float32), grad_w_out.astype(jnp.float32))
```

```python
import math
import jax
import jax.numpy as jnp
import numpy as np
from jax import lax
from jax.experimental import pallas as pl
from jax.experimental.pallas import tpu as pltpu
from jax.sharding import PartitionSpec as P

HEAD_DIM = 128
NORM_EPS = 1.0e-5
ROPE_BASE = 10000.0
MASK_VALUE = -1.0e30
SCORE_SCALE = 1.0 / math.sqrt(HEAD_DIM)
EXP2_SCALE = SCORE_SCALE * math.log2(math.e)
ROWS = 256
BF16 = jnp.bfloat16
F32 = jnp.float32


def dot(a, b, contract):
    return lax.dot_general(a, b, ((contract[:1], contract[1:]), ((), ())), preferred_element_type=F32)


def rope_tables(seq_len):
    inv_freq = ROPE_BASE ** (-np.arange(0, HEAD_DIM, 2, dtype=np.float64) / HEAD_DIM)
    angles = np.arange(seq_len, dtype=np.float64)[:, None] * inv_freq[None, :]
    cos_t = np.repeat(np.cos(angles), 2, axis=1)
    sin_t = np.stack([-np.sin(angles), np.sin(angles)], axis=-1).reshape(seq_len, HEAD_DIM)
    return cos_t.astype(np.float32), sin_t.astype(np.float32)


def rotate(t, cos_t, sin_t):
    even = lax.broadcasted_iota(jnp.int32, t.shape, 1) % 2 == 0
    swapped = jnp.where(even, pltpu.roll(t, HEAD_DIM - 1, 1), pltpu.roll(t, 1, 1))
    return t * cos_t + swapped * sin_t


def proj_kernel(x_ref, dout_ref, gain_ref, wqkv_ref, wo_ref, cos_ref, sin_ref, n_ref, q_ref, k_ref, v_ref, do_ref):
    x = x_ref[...].astype(F32)
    inv = lax.rsqrt(jnp.mean(x * x, axis=-1, keepdims=True) + NORM_EPS)
    n = (x * inv * gain_ref[...]).astype(BF16)
    n_ref[...] = n
    qkv = dot(n, wqkv_ref[...], (1, 0))
    cos_t, sin_t = cos_ref[...], sin_ref[...]
    q_ref[:, :HEAD_DIM] = rotate(qkv[:, :HEAD_DIM], cos_t, sin_t).astype(BF16)
    q_ref[:, HEAD_DIM:] = rotate(qkv[:, HEAD_DIM:2 * HEAD_DIM], cos_t, sin_t).astype(BF16)
    k_ref[...] = rotate(qkv[:, 2 * HEAD_DIM:3 * HEAD_DIM], cos_t, sin_t).astype(BF16)
    v_ref[...] = qkv[:, 3 * HEAD_DIM:].astype(BF16)
    do_ref[...] = dot(dout_ref[...], wo_ref[...], (1, 1)).astype(BF16)


def project(x, dout, gain, wqkv, wo, cos_t, sin_t):
    seq, d = x.shape
    row = lambda w: pl.BlockSpec((ROWS, w), lambda i: (i, 0))
    whole = lambda a: pl.BlockSpec(a.shape, lambda i: (0, 0))
    widths = (d, 2 * HEAD_DIM, HEAD_DIM, HEAD_DIM, 2 * HEAD_DIM)
    return pl.pallas_call(
        proj_kernel, grid=(seq // ROWS,),
        in_specs=[row(d), row(d), whole(gain), whole(wqkv), whole(wo), row(HEAD_DIM), row(HEAD_DIM)],
        out_specs=[row(w) for w in widths],
        out_shape=[jax.ShapeDtypeStruct((seq, w), BF16) for w in widths],
        cost_estimate=pl.CostEstimate(flops=2 * seq * d * 6 * HEAD_DIM, bytes_accessed=6 * seq * d, transcendentals=0),
        name='project')(x, dout, gain, wqkv, wo, cos_t, sin_t)


def stack_heads(ref, rows):
    return jnp.concatenate([ref[rows, :HEAD_DIM], ref[rows, HEAD_DIM:]], axis=0)


def attn_fwd_kernel(q_ref, k_ref, v_ref, o_ref):
    seq = q_ref.shape[0]
    row_id = lax.broadcasted_iota(jnp.int32, (2 * ROWS, ROWS), 0) % ROWS
    causal = row_id >= lax.broadcasted_iota(jnp.int32, (2 * ROWS, ROWS), 1)
    for i in range(seq // ROWS):
        lo = i * ROWS
        rows = pl.ds(lo, ROWS)
        q2 = stack_heads(q_ref, rows)
        s_diag = jnp.where(causal, dot(q2, k_ref[rows, :], (1, 1)), MASK_VALUE)
        m = jnp.max(s_diag, axis=-1, keepdims=True)
        if lo:
            s_pre = dot(q2, k_ref[:lo, :], (1, 1))
            m = jnp.maximum(m, jnp.max(s_pre, axis=-1, keepdims=True))
        p_diag = jnp.exp2((s_diag - m) * EXP2_SCALE)
        total = jnp.sum(p_diag, axis=-1, keepdims=True)
        if lo:
            p_pre = jnp.exp2((s_pre - m) * EXP2_SCALE)
            total = total + jnp.sum(p_pre, axis=-1, keepdims=True)
        scale = 1.0 / total
        o2 = dot((p_diag * scale).astype(BF16), v_ref[rows, :], (1, 0))
        if lo:
            o2 = o2 + dot((p_pre * scale).astype(BF16), v_ref[:lo, :], (1, 0))
        o_ref[rows, :HEAD_DIM] = o2[:ROWS].astype(BF16)
        o_ref[rows, HEAD_DIM:] = o2[ROWS:].astype(BF16)


def attn_fwd(q, k, v):
    seq = q.shape[0]
    return pl.pallas_call(
        attn_fwd_kernel,
        out_shape=jax.ShapeDtypeStruct(q.shape, BF16),
        compiler_params=pltpu.CompilerParams(vmem_limit_bytes=48 * 2**20),
        cost_estimate=pl.CostEstimate(flops=4 * seq * seq * HEAD_DIM, bytes_accessed=8 * seq * HEAD_DIM, transcendentals=seq * seq),
        name='attn_fwd')(q, k, v)


def attn_bwd_rows(i, q_ref, k_ref, v_ref, do_ref, cos_ref, sin_ref, dq_ref, dk_acc, dv_acc):
    lo, hi = i * ROWS, (i + 1) * ROWS
    rows = pl.ds(lo, ROWS)
    q2, do2 = stack_heads(q_ref, rows), stack_heads(do_ref, rows)
    k_all, v_all = k_ref[:hi, :], v_ref[:hi, :]
    key_id = lax.broadcasted_iota(jnp.int32, (ROWS, 2 * ROWS), 0)
    causal = key_id <= lax.broadcasted_iota(jnp.int32, (ROWS, 2 * ROWS), 1) % ROWS
    s_t = dot(k_all, q2, (1, 1))
    s_diag = jnp.where(causal, s_t[lo:], MASK_VALUE)
    s_t = jnp.concatenate([s_t[:lo], s_diag], axis=0) if lo else s_diag
    m = jnp.max(s_t, axis=0, keepdims=True)
    p = jnp.exp2((s_t - m) * EXP2_SCALE)
    p = p * (1.0 / jnp.sum(p, axis=0, keepdims=True))
    dp = dot(v_all, do2, (1, 1))
    delta = jnp.sum(p * dp, axis=0, keepdims=True)
    ds = (p * (dp - delta) * SCORE_SCALE).astype(BF16)
    dv = dot(p.astype(BF16), do2, (1, 0))
    dk = dot(ds, q2, (1, 0))
    dq2 = dot(ds, k_all, (0, 0))
    if lo:
        dk_acc[:lo, :] += dk[:lo]
        dv_acc[:lo, :] += dv[:lo]
    dk_acc[lo:hi, :] = dk[lo:]
    dv_acc[lo:hi, :] = dv[lo:]
    cos_t, sin_t = cos_ref[rows, :], sin_ref[rows, :]
    dq_ref[rows, :HEAD_DIM] = rotate(dq2[:ROWS], cos_t, -sin_t).astype(BF16)
    dq_ref[rows, HEAD_DIM:] = rotate(dq2[ROWS:], cos_t, -sin_t).astype(BF16)


def attn_bwd_kernel(q_ref, k_ref, v_ref, do_ref, cos_ref, sin_ref, dq_ref, dkv_ref, dk_acc):
    seq = q_ref.shape[0]
    dv_acc = dkv_ref.at[:, pl.ds(HEAD_DIM, HEAD_DIM)]
    for i in range(seq // ROWS):
        attn_bwd_rows(i, q_ref, k_ref, v_ref, do_ref, cos_ref, sin_ref, dq_ref, dk_acc, dv_acc)
    dkv_ref[:, :HEAD_DIM] = rotate(dk_acc[...], cos_ref[...], -sin_ref[...])


def attn_bwd(q, k, v, do, cos_t, sin_t):
    seq = q.shape[0]
    return pl.pallas_call(
        attn_bwd_kernel,
        out_shape=[jax.ShapeDtypeStruct(q.shape, BF16), jax.ShapeDtypeStruct((seq, 2 * HEAD_DIM), F32)],
        scratch_shapes=[pltpu.VMEM((seq, HEAD_DIM), F32)],
        compiler_params=pltpu.CompilerParams(vmem_limit_bytes=56 * 2**20),
        cost_estimate=pl.CostEstimate(flops=10 * seq * seq * HEAD_DIM, bytes_accessed=16 * seq * HEAD_DIM, transcendentals=seq * seq),
        name='attn_bwd')(q, k, v, do, cos_t, sin_t)


def group_sum(tensor, tp_size, group_size):
    total = tensor
    for level in range(group_size.bit_length() - 1):
        distance = 2 ** level
        partner_pairs = [(source, source ^ distance) for source in range(tp_size)]
        total = total + lax.ppermute(total, 'tp', perm=partner_pairs)
    return total


def solution(mesh):
    tp_size = mesh.shape['tp']

    def block_fn(hidden, grad_out, norm_gain, w_query, w_key, w_value, w_out):
        kv_heads = w_key.shape[1] // HEAD_DIM
        group_size = tp_size // kv_heads
        batch, seq_len, d_model = hidden.shape
        kv_index = lax.axis_index('tp') // group_size
        w_k = lax.dynamic_slice_in_dim(w_key, kv_index * HEAD_DIM, HEAD_DIM, axis=1)
        w_v = lax.dynamic_slice_in_dim(w_value, kv_index * HEAD_DIM, HEAD_DIM, axis=1)
        w_qkv = jnp.concatenate([w_query, w_k, w_v], axis=1)
        cos_t, sin_t = rope_tables(seq_len)
        x, dout = hidden[0], grad_out[0]
        gain = norm_gain.astype(F32)[None, :]

        n, q, k, v, do = project(x, dout, gain, w_qkv, w_out, cos_t, sin_t)
        o = attn_fwd(q, k, v)
        out_part = dot(o, w_out, (1, 0))
        attn_sum = lax.psum(out_part, 'tp')
        x32 = x.astype(F32)
        block_out = (x32 + attn_sum).astype(BF16)

        dq, dkv_part = attn_bwd(q, k, v, do, cos_t, sin_t)
        dkv = group_sum(dkv_part, tp_size, group_size)
        d_all = jnp.concatenate([dq, (dkv_part).astype(BF16)], axis=1)
        dn_part = dot(d_all, w_qkv, (1, 1))
        dn_part, attn_sum = lax.optimization_barrier((dn_part, attn_sum))
        dn = lax.psum(dn_part, 'tp')
        grad_w_out = dot(o, dout, (0, 0))
        grad_w_query = dot(n, dq, (0, 0))
        dkv = dkv.astype(BF16)
        grad_w_key = dot(n, dkv[:, :HEAD_DIM], (0, 0))
        grad_w_value = dot(n, dkv[:, HEAD_DIM:], (0, 0))
        inv = lax.rsqrt(jnp.mean(x32 * x32, axis=-1, keepdims=True) + NORM_EPS)
        unit = x32 * inv
        scaled = dn * gain
        grad_hidden = (dout.astype(F32) + inv * (scaled - unit * jnp.mean(scaled * unit, axis=-1, keepdims=True))).astype(BF16)
        grad_gain = jnp.sum(dn * unit, axis=0)
        return block_out[None], grad_hidden[None], grad_gain, grad_w_query, grad_w_key, grad_w_value, grad_w_out

    act_spec = P('dp', None, None)
    return jax.shard_map(
        block_fn, mesh=mesh,
        in_specs=(act_spec, act_spec, P(None), P(None, 'tp'), P(None, None), P(None, None), P('tp', None)),
        out_specs=(act_spec, act_spec, P('dp'), P('dp', 'tp'), P('dp', 'tp'), P('dp', 'tp'), P(('dp', 'tp'), None)),
        check_vma=False)
```

```python
import functools
import math
import jax
import jax.numpy as jnp
import numpy as np
from jax import lax
from jax.experimental import pallas as pl
from jax.experimental.pallas import tpu as pltpu
from jax.sharding import PartitionSpec as P

HEAD_DIM = 128
NORM_EPS = 1.0e-5
ROPE_BASE = 10000.0
MASK_VALUE = -1.0e30
SCORE_SCALE = 1.0 / math.sqrt(HEAD_DIM)
EXP2_SCALE = SCORE_SCALE * math.log2(math.e)
ROWS = 256
BF16 = jnp.bfloat16
F32 = jnp.float32
VMEM_LIMIT = 66 * 10**6


def dot(a, b, contract):
    return lax.dot_general(a, b, ((contract[:1], contract[1:]), ((), ())), preferred_element_type=F32)


def rope_tables(seq_len):
    inv_freq = ROPE_BASE ** (-np.arange(0, HEAD_DIM, 2, dtype=np.float64) / HEAD_DIM)
    angles = np.arange(seq_len, dtype=np.float64)[:, None] * inv_freq[None, :]
    cos_t = np.repeat(np.cos(angles), 2, axis=1)
    sin_t = np.stack([-np.sin(angles), np.sin(angles)], axis=-1).reshape(seq_len, HEAD_DIM)
    return cos_t.astype(np.float32), sin_t.astype(np.float32)


def rotate(t, cos_t, sin_t):
    even = lax.broadcasted_iota(jnp.int32, t.shape, 1) % 2 == 0
    swapped = jnp.where(even, pltpu.roll(t, HEAD_DIM - 1, 1), pltpu.roll(t, 1, 1))
    return t * cos_t + swapped * sin_t


def proj_kernel(x_ref, dout_ref, gain_ref, wqkv_ref, wo_ref, cos_ref, sin_ref, n_ref, q_ref, k_ref, v_ref, do_ref):
    x = x_ref[...].astype(F32)
    inv = lax.rsqrt(jnp.mean(x * x, axis=-1, keepdims=True) + NORM_EPS)
    n = (x * inv * gain_ref[...]).astype(BF16)
    n_ref[...] = n
    qkv = dot(n, wqkv_ref[...], (1, 0))
    cos_t, sin_t = cos_ref[...], sin_ref[...]
    q_ref[:, :HEAD_DIM] = rotate(qkv[:, :HEAD_DIM], cos_t, sin_t).astype(BF16)
    q_ref[:, HEAD_DIM:] = rotate(qkv[:, HEAD_DIM:2 * HEAD_DIM], cos_t, sin_t).astype(BF16)
    k_ref[...] = rotate(qkv[:, 2 * HEAD_DIM:3 * HEAD_DIM], cos_t, sin_t).astype(BF16)
    v_ref[...] = qkv[:, 3 * HEAD_DIM:].astype(BF16)
    do_ref[...] = dot(dout_ref[...], wo_ref[...], (1, 1)).astype(BF16)


def project(x, dout, gain, wqkv, wo, cos_t, sin_t):
    seq, d = x.shape
    row = lambda w: pl.BlockSpec((ROWS, w), lambda i: (i, 0))
    whole = lambda a: pl.BlockSpec(a.shape, lambda i: (0, 0))
    widths = (d, 2 * HEAD_DIM, HEAD_DIM, HEAD_DIM, 2 * HEAD_DIM)
    return pl.pallas_call(
        proj_kernel, grid=(seq // ROWS,),
        in_specs=[row(d), row(d), whole(gain), whole(wqkv), whole(wo), row(HEAD_DIM), row(HEAD_DIM)],
        out_specs=[row(w) for w in widths],
        out_shape=[jax.ShapeDtypeStruct((seq, w), BF16) for w in widths],
        cost_estimate=pl.CostEstimate(flops=2 * seq * d * 6 * HEAD_DIM, bytes_accessed=6 * seq * d, transcendentals=0),
        name='project')(x, dout, gain, wqkv, wo, cos_t, sin_t)


def stack_heads(ref, rows):
    return jnp.concatenate([ref[rows, :HEAD_DIM], ref[rows, HEAD_DIM:]], axis=0)


def attn_fwd_kernel(q_ref, k_ref, v_ref, o_ref, o32_ref):
    seq = q_ref.shape[0]
    row_id = lax.broadcasted_iota(jnp.int32, (2 * ROWS, ROWS), 0) % ROWS
    causal = row_id >= lax.broadcasted_iota(jnp.int32, (2 * ROWS, ROWS), 1)
    for i in range(seq // ROWS):
        lo = i * ROWS
        rows = pl.ds(lo, ROWS)
        q2 = stack_heads(q_ref, rows)
        s_diag = jnp.where(causal, dot(q2, k_ref[rows, :], (1, 1)), MASK_VALUE)
        m = jnp.max(s_diag, axis=-1, keepdims=True)
        if lo:
            s_pre = dot(q2, k_ref[:lo, :], (1, 1))
            m = jnp.maximum(m, jnp.max(s_pre, axis=-1, keepdims=True))
        p_diag = jnp.exp2((s_diag - m) * EXP2_SCALE)
        total = jnp.sum(p_diag, axis=-1, keepdims=True)
        if lo:
            p_pre = jnp.exp2((s_pre - m) * EXP2_SCALE)
            total = total + jnp.sum(p_pre, axis=-1, keepdims=True)
        scale = 1.0 / total
        o2 = dot((p_diag * scale).astype(BF16), v_ref[rows, :], (1, 0))
        if lo:
            o2 = o2 + dot((p_pre * scale).astype(BF16), v_ref[:lo, :], (1, 0))
        o2 = o2.astype(BF16)
        for head in range(2):
            cols = slice(head * HEAD_DIM, (head + 1) * HEAD_DIM)
            o_ref[rows, cols] = o2[head * ROWS:(head + 1) * ROWS]
            o32_ref[rows, cols] = o2[head * ROWS:(head + 1) * ROWS].astype(F32)


def attn_fwd(q, k, v):
    seq = q.shape[0]
    return pl.pallas_call(
        attn_fwd_kernel,
        out_shape=[jax.ShapeDtypeStruct(q.shape, BF16), jax.ShapeDtypeStruct(q.shape, F32)],
        compiler_params=pltpu.CompilerParams(vmem_limit_bytes=48 * 2**20),
        cost_estimate=pl.CostEstimate(flops=4 * seq * seq * HEAD_DIM, bytes_accessed=8 * seq * HEAD_DIM, transcendentals=seq * seq),
        name='attn_fwd')(q, k, v)


def attn_bwd_rows(i, head, q_ref, k_ref, v_ref, do_ref, cos_ref, sin_ref, dq_ref, dq32_ref, dk_acc, dv_acc):
    lo, hi = i * ROWS, (i + 1) * ROWS
    rows, cols = pl.ds(lo, ROWS), pl.ds(head * HEAD_DIM, HEAD_DIM)
    q, do = q_ref[rows, cols], do_ref[rows, cols]
    k_all, v_all = k_ref[:hi, :], v_ref[:hi, :]
    causal = lax.broadcasted_iota(jnp.int32, (ROWS, ROWS), 0) <= lax.broadcasted_iota(jnp.int32, (ROWS, ROWS), 1)
    s_t = dot(k_all, q, (1, 1))
    s_diag = jnp.where(causal, s_t[lo:], MASK_VALUE)
    s_t = jnp.concatenate([s_t[:lo], s_diag], axis=0) if lo else s_diag
    m = jnp.max(s_t, axis=0, keepdims=True)
    p = jnp.exp2((s_t - m) * EXP2_SCALE)
    p = p * (1.0 / jnp.sum(p, axis=0, keepdims=True))
    dp = dot(v_all, do, (1, 1))
    delta = jnp.sum(p * dp, axis=0, keepdims=True)
    ds = (p * (dp - delta) * SCORE_SCALE).astype(BF16)
    dv = dot(p.astype(BF16), do, (1, 0))
    dk = dot(ds, q, (1, 0))
    dq = dot(ds, k_all, (0, 0))
    if head == 0:
        dk_acc[lo:hi, :] = dk[lo:]
        dv_acc[lo:hi, :] = dv[lo:]
        if lo:
            dk_acc[:lo, :] += dk[:lo]
            dv_acc[:lo, :] += dv[:lo]
    else:
        dk_acc[:hi, :] += dk
        dv_acc[:hi, :] += dv
    dq = rotate(dq, cos_ref[rows, :], -sin_ref[rows, :]).astype(BF16)
    dq_ref[rows, cols] = dq
    dq32_ref[rows, cols] = dq.astype(F32)


SUBS = 2


def ring_kernel_setup(n):
    me = lax.axis_index('tp')
    chip, core = me // 2, me % 2
    right = (chip + 1) % n * 2 + core
    left = (chip + n - 1) % n * 2 + core
    sib = me + 1 - 2 * core
    barrier = pltpu.get_barrier_semaphore()
    for peer in (right, left, sib):
        pl.semaphore_signal(barrier, inc=1, device_id={'tp': peer}, device_id_type=pl.DeviceIdType.MESH)
    pl.semaphore_wait(barrier, 3)
    return chip, core, right, left, sib


def remote(src, dst, send, recv, peer):
    return pltpu.make_async_remote_copy(src_ref=src, dst_ref=dst, send_sem=send, recv_sem=recv,
                                        device_id={'tp': peer}, device_id_type=pl.DeviceIdType.MESH)


def ring_sum(n, place, extra, partial, finish, rider, out_ref, gain_acc, bufs, sems):
    chip, core, right, left, sib = place
    rs_buf, ag_buf, sib_buf, obuf = bufs
    rs_send, rs_recv, ag_send, ag_recv, sib_send, sib_recv, out_sem, credit = sems
    width = rs_buf.shape[-1]
    block = out_ref.shape[0] // n
    sub_rows = block // SUBS
    half = 2 * width
    peers = (right, left)

    def part(slot_ref, sub, with_extra):
        return slot_ref.at[pl.ds(sub * sub_rows, sub_rows + (extra if with_extra and sub == SUBS - 1 else 0)), :]

    def rs_copy(s, sub, way):
        return remote(part(rs_buf.at[way, s], sub, False), part(rs_buf.at[way, s + 1], sub, False),
                      rs_send.at[way, s, sub], rs_recv.at[way, s, sub], peers[way])

    def ag_copy(s, sub, way):
        return remote(part(ag_buf.at[way, s], sub, True), part(ag_buf.at[way, s + 1], sub, True),
                      ag_send.at[way, s, sub], ag_recv.at[way, s, sub], peers[way])

    def sib_copy(s, sub, way):
        rows = sub_rows + (extra if sub == SUBS - 1 else 0)
        k = SUBS * s + sub
        return remote(part(ag_buf.at[way, s], sub, True), sib_buf.at[way, k % 4, pl.ds(0, rows), :],
                      sib_send.at[way, k], sib_recv.at[way, k], sib)

    def my_part(dest, sub, way):
        row = pl.multiple_of(dest * block + sub * sub_rows, sub_rows)
        return partial(pl.ds(row, sub_rows), way)

    def dest_of(s, way):
        return (chip + n - 1 - s) % n if way == 0 else (chip + 1 + s) % n

    def local(ref, sub):
        return pl.ds(sub * sub_rows, sub_rows)

    for sub in range(SUBS):
        for way in range(2):
            rs_buf[way, 0, local(rs_buf, sub), :] = my_part(dest_of(0, way), sub, way)
            rs_copy(0, sub, way).start()
    rider(0)

    def rs_step(s, carry):
        for sub in range(SUBS):
            for way in range(2):
                rs_copy(s - 1, sub, way).wait_recv()
                rs_buf[way, s, local(rs_buf, sub), :] += my_part(dest_of(s, way), sub, way)
                rs_copy(s, sub, way).start()
            if sub == 0:
                rider(s)
        return carry

    lax.fori_loop(1, n - 1, rs_step, 0)
    for sub in range(SUBS):
        for way in range(2):
            rs_copy(n - 2, sub, way).wait_recv()
        finish(sub, [rs_buf[way, n - 1, local(rs_buf, sub), :] + my_part(chip, sub, way) for way in range(2)])

    def out_copy(whose, s, sub, way):
        b = (chip + n - s) % n if way == 0 else (chip + s) % n
        col = (core if whose == 0 else 1 - core) * half + way * width
        dst = out_ref.at[pl.ds(pl.multiple_of(b * block + sub * sub_rows, sub_rows), sub_rows), pl.ds(pl.multiple_of(col, 128), width)]
        return pltpu.make_async_copy(obuf.at[whose, sub, way], dst, out_sem.at[whose, sub, way])

    def emit(whose, s, sub, way, values):
        @pl.when(s >= 1)
        def _():
            out_copy(whose, s - 1, sub, way).wait()
        obuf[whose, sub, way] = values.astype(BF16)
        out_copy(whose, s, sub, way).start()

    def own_chunk(s, sub, forward):
        @pl.when(s >= 2)
        def _():
            pl.semaphore_wait(credit, 1)
        for way in range(2):
            if forward:
                ag_copy(s, sub, way).start()
            sib_copy(s, sub, way).start()
        for way in range(2):
            emit(0, s, sub, way, ag_buf[way, s, local(ag_buf, sub), :])
            if extra and sub == SUBS - 1:
                gain_acc[0, way] += ag_buf[way, s, pl.ds(block, extra), :]

    def sib_chunk(s, sub):
        k = SUBS * s + sub
        for way in range(2):
            sib_copy(s, sub, way).wait_recv()
            emit(1, s, sub, way, sib_buf[way, k % 4, pl.ds(0, sub_rows), :])
            if extra and sub == SUBS - 1:
                gain_acc[1, way] += sib_buf[way, k % 4, pl.ds(sub_rows, extra), :]

        @pl.when(s < n - 2)
        def _():
            pl.semaphore_signal(credit, inc=1, device_id={'tp': sib}, device_id_type=pl.DeviceIdType.MESH)

    own_chunk(0, 0, True)
    own_chunk(0, 1, True)
    rider(n - 1)
    sib_chunk(0, 0)

    def ag_step(s, carry):
        for sub in range(SUBS):
            for way in range(2):
                ag_copy(s - 1, sub, way).wait_recv()
            own_chunk(s, sub, True)
            if sub == 0:
                sib_chunk(s - 1, 1)
            else:
                sib_chunk(s, 0)
        return carry

    lax.fori_loop(1, n - 1, ag_step, 0)
    last = n - 1
    for sub in range(SUBS):
        for way in range(2):
            ag_copy(last - 1, sub, way).wait_recv()
        own_chunk(last, sub, False)
        if sub == 0:
            sib_chunk(last - 1, 1)
        else:
            sib_chunk(last, 0)
    sib_chunk(last, 1)
    for sub in range(SUBS):
        for way in range(2):
            for whose in range(2):
                out_copy(whose, last, sub, way).wait()

    def drain(s, carry):
        for sub in range(SUBS):
            for way in range(2):
                rs_copy(s, sub, way).wait_send()
                ag_copy(s, sub, way).wait_send()
                sib_copy(s, sub, way).wait_send()
        return carry

    lax.fori_loop(0, n - 1, drain, 0)
    for sub in range(SUBS):
        for way in range(2):
            sib_copy(last, sub, way).wait_send()


def ring_scratch(n, seq, d_model, extra):
    width, block = d_model // 4, seq // n
    sub_rows = block // SUBS
    dma = pltpu.SemaphoreType.DMA
    return [
        pltpu.VMEM((2, n, block, width), F32),
        pltpu.VMEM((2, n, block + extra, width), F32),
        pltpu.VMEM((2, 4, sub_rows + extra, width), F32),
        pltpu.VMEM((2, SUBS, 2, sub_rows, width), BF16),
        dma((2, n - 1, SUBS)), dma((2, n - 1, SUBS)), dma((2, n - 1, SUBS)), dma((2, n - 1, SUBS)),
        dma((2, SUBS * n)), dma((2, SUBS * n)), dma((2, SUBS, 2)), pltpu.SemaphoreType.REGULAR,
    ]


def out_kernel(n, riders, o_ref, osib_ref, wo_ref, wosib_ref, x_ref, q_ref, k_ref, v_ref, do_ref, cos_ref, sin_ref,
               out_ref, dq_ref, dq32_ref, dkv_ref, lhs, rhs, x_rows, dk_acc, row_sem, *ring):
    bufs, sems = ring[:4], ring[4:]
    place = ring_kernel_setup(n)
    chip, core = place[:2]
    width = bufs[0].shape[-1]
    block = x_rows.shape[0]
    inner = o_ref.shape[1]
    x_copy = pltpu.make_async_copy(
        x_ref.at[pl.ds(pl.multiple_of(chip * block, block), block), pl.ds(pl.multiple_of(core * 2 * width, 128), 2 * width)],
        x_rows, row_sem)
    x_copy.start()
    lhs[:, :inner] = o_ref[...]
    lhs[:, inner:] = osib_ref[...].astype(BF16)
    rhs[:inner, :] = wo_ref[...]
    rhs[inner:, :] = wosib_ref[...].astype(BF16)

    def partial(rows, way):
        return dot(lhs[rows, :], rhs[:, way * width:(way + 1) * width], (1, 0))

    sub_rows = block // SUBS

    def finish(sub, sums):
        if sub == 0:
            x_copy.wait()
        for way in range(2):
            rows = pl.ds(sub * sub_rows, sub_rows)
            bufs[1][way, 0, rows, :] = sums[way] + x_rows[rows, way * width:(way + 1) * width].astype(F32)

    dv_acc = dkv_ref.at[:, pl.ds(HEAD_DIM, HEAD_DIM)]
    count = q_ref.shape[0] // ROWS

    def ride(step):
        for i in range(step * count // n, (step + 1) * count // n):
            for head in range(2):
                attn_bwd_rows(i, head, q_ref, k_ref, v_ref, do_ref, cos_ref, sin_ref, dq_ref, dq32_ref, dk_acc, dv_acc)
        if step == n - 1:
            dkv_ref[:, :HEAD_DIM] = rotate(dk_acc[...], cos_ref[...], -sin_ref[...])

    def rider(step):
        if not riders:
            return
        if isinstance(step, int):
            ride(step)
        else:
            for static in range(1, n - 1):
                pl.when(step == static)(lambda static=static: ride(static))

    ring_sum(n, place, 0, partial, finish, rider, out_ref, None, bufs, sems)


def grad_kernel(n, dq_ref, dqsib_ref, dkv_ref, dkvsib_ref, wq_ref, wqsib_ref, wkv_ref, x_ref, dout_ref, gain_ref,
                out_ref, gsum_ref, lhs, rhs, x_rows, dout_rows, unit_buf, stat_buf, gain_acc, row_sem, stat_send, stat_recv, *ring):
    bufs, sems = ring[:4], ring[4:]
    place = ring_kernel_setup(n)
    chip, core, right, left, sib = place
    width = bufs[0].shape[-1]
    block = x_rows.shape[0]
    inner = dq_ref.shape[1]
    half = 2 * width
    row = pl.multiple_of(chip * block, block)
    col = pl.multiple_of(core * half, 128)
    x_copy = pltpu.make_async_copy(x_ref.at[pl.ds(row, block), :], x_rows, row_sem.at[0])
    dout_copy = pltpu.make_async_copy(dout_ref.at[pl.ds(row, block), pl.ds(col, half)], dout_rows, row_sem.at[1])
    x_copy.start()
    dout_copy.start()
    lhs[:, :inner] = dq_ref[...]
    lhs[:, inner:2 * inner] = dqsib_ref[...].astype(BF16)
    lhs[:, 2 * inner:] = (dkv_ref[...] + dkvsib_ref[...]).astype(BF16)
    rhs[:, :inner] = wq_ref[...]
    rhs[:, inner:2 * inner] = wqsib_ref[...].astype(BF16)
    rhs[:, 2 * inner:] = wkv_ref[...]
    gain_acc[...] = jnp.zeros_like(gain_acc)

    def partial(rows, way):
        return dot(lhs[rows, :], rhs[way * width:(way + 1) * width, :], (1, 1))

    sub_rows = block // SUBS

    def prepare(sub):
        rows = pl.ds(sub * sub_rows, sub_rows)
        x = x_rows[rows, :].astype(F32)
        inv = lax.rsqrt(jnp.mean(x * x, axis=-1, keepdims=True) + NORM_EPS)
        stat_buf[2, rows, :] = jnp.broadcast_to(inv, (sub_rows, HEAD_DIM))
        mine = x_rows[rows, pl.ds(col, half)].astype(F32)
        unit_buf[rows, :] = mine * inv

    def rider(step):
        if isinstance(step, int) and step == 0:
            x_copy.wait()
            dout_copy.wait()
            for sub in range(SUBS):
                prepare(sub)

    def stat_copy(sub):
        rows = pl.ds(sub * sub_rows, sub_rows)
        return remote(stat_buf.at[0, rows, :], stat_buf.at[1, rows, :], stat_send.at[sub], stat_recv.at[sub], sib)

    def finish(sub, sums):
        rows = pl.ds(sub * sub_rows, sub_rows)
        ag_buf = bufs[1]
        total = jnp.zeros((sub_rows, 1), F32)
        for way in range(2):
            cols = slice(way * width, (way + 1) * width)
            unit = unit_buf[rows, cols]
            prod = sums[way] * unit
            total = total + jnp.sum(prod * gain_ref[:, cols], axis=-1, keepdims=True)
            gsum = jnp.sum(prod.reshape(sub_rows // 8, 8, width), axis=0)
            ag_buf[way, 0, pl.ds(block, 8), :] = gsum if sub == 0 else gsum + ag_buf[way, 0, pl.ds(block, 8), :]
            ag_buf[way, 0, rows, :] = sums[way]
        stat_buf[0, rows, :] = jnp.broadcast_to(total, (sub_rows, HEAD_DIM))
        stat_copy(sub).start()
        stat_copy(sub).wait()
        mean = (stat_buf[0, rows, 0:1] + stat_buf[1, rows, 0:1]) * (1.0 / (2 * half))
        inv = stat_buf[2, rows, 0:1]
        for way in range(2):
            cols = slice(way * width, (way + 1) * width)
            scaled = ag_buf[way, 0, rows, :] * gain_ref[:, cols]
            ag_buf[way, 0, rows, :] = dout_rows[rows, cols].astype(F32) + inv * (scaled - unit_buf[rows, cols] * mean)

    ring_sum(n, place, 8, partial, finish, rider, out_ref, gain_acc, bufs, sems)
    for way in range(2):
        gsum_ref[core, way] = jnp.sum(gain_acc[0, way], axis=0, keepdims=True)
        gsum_ref[1 - core, way] = jnp.sum(gain_acc[1, way], axis=0, keepdims=True)


def out_sum(n, o, o_sib, wo, wo_sib, x, q, k, v, do, cos_t, sin_t):
    seq, d_model = x.shape
    half = d_model // 2
    vmem, hbm = pl.BlockSpec(memory_space=pltpu.VMEM), pl.BlockSpec(memory_space=pl.ANY)
    shape = jax.ShapeDtypeStruct
    return pl.pallas_call(
        functools.partial(out_kernel, n, True),
        out_shape=[shape((seq, d_model), BF16), shape(q.shape, BF16), shape(q.shape, F32), shape((seq, 2 * HEAD_DIM), F32)],
        in_specs=[vmem] * 4 + [hbm] + [vmem] * 6, out_specs=[hbm] + [vmem] * 3,
        scratch_shapes=[pltpu.VMEM((seq, 2 * o.shape[1]), BF16), pltpu.VMEM((2 * o.shape[1], half), BF16),
                        pltpu.VMEM((seq // n, half), BF16), pltpu.VMEM((seq, HEAD_DIM), F32), pltpu.SemaphoreType.DMA]
        + ring_scratch(n, seq, d_model, 0),
        compiler_params=pltpu.CompilerParams(collective_id=1, has_side_effects=True, vmem_limit_bytes=VMEM_LIMIT),
        cost_estimate=pl.CostEstimate(flops=10 * seq * seq * HEAD_DIM, bytes_accessed=4 * seq * d_model, transcendentals=seq * seq),
        name='out_sum')(o, o_sib, wo, wo_sib, x, q, k, v, do, cos_t, sin_t)


def grad_sum(n, dq, dq_sib, dkv, dkv_sib, wq, wq_sib, wkv, x, dout, gain):
    seq, d_model = x.shape
    half, block, width = d_model // 2, seq // n, d_model // 4
    kdim = 2 * dq.shape[1] + dkv.shape[1]
    vmem, hbm = pl.BlockSpec(memory_space=pltpu.VMEM), pl.BlockSpec(memory_space=pl.ANY)
    shape = jax.ShapeDtypeStruct
    dma = pltpu.SemaphoreType.DMA
    return pl.pallas_call(
        functools.partial(grad_kernel, n),
        out_shape=[shape((seq, d_model), BF16), shape((2, 2, 1, width), F32)],
        in_specs=[vmem] * 7 + [hbm] * 2 + [vmem], out_specs=[hbm, vmem],
        scratch_shapes=[pltpu.VMEM((seq, kdim), BF16), pltpu.VMEM((half, kdim), BF16),
                        pltpu.VMEM((block, d_model), BF16), pltpu.VMEM((block, half), BF16), pltpu.VMEM((block, half), F32),
                        pltpu.VMEM((3, block, HEAD_DIM), F32), pltpu.VMEM((2, 2, 8, width), F32),
                        dma((2,)), dma((SUBS,)), dma((SUBS,))]
        + ring_scratch(n, seq, d_model, 8),
        compiler_params=pltpu.CompilerParams(collective_id=2, has_side_effects=True, vmem_limit_bytes=VMEM_LIMIT),
        cost_estimate=pl.CostEstimate(flops=4 * seq * kdim * half, bytes_accessed=4 * seq * d_model, transcendentals=0),
        name='grad_sum')(dq, dq_sib, dkv, dkv_sib, wq, wq_sib, wkv, x, dout, gain)


def solution(mesh):
    tp_size = mesh.shape['tp']
    chips = tp_size // 2
    swap = [(source, source ^ 1) for source in range(tp_size)]

    def block_fn(hidden, grad_out, norm_gain, w_query, w_key, w_value, w_out):
        batch, seq_len, d_model = hidden.shape
        half = d_model // 2
        tp_index = lax.axis_index('tp')
        kv_index, core = tp_index // 2, tp_index % 2
        w_k = lax.dynamic_slice_in_dim(w_key, kv_index * HEAD_DIM, HEAD_DIM, axis=1)
        w_v = lax.dynamic_slice_in_dim(w_value, kv_index * HEAD_DIM, HEAD_DIM, axis=1)
        w_qkv = jnp.concatenate([w_query, w_k, w_v], axis=1)
        cos_t, sin_t = rope_tables(seq_len)
        x, dout = hidden[0], grad_out[0]
        gain = norm_gain.astype(F32)[None, :]
        mine, other = core * half, (1 - core) * half
        wo_mine = lax.dynamic_slice_in_dim(w_out, mine, half, axis=1)
        wo_sib = lax.ppermute(lax.dynamic_slice_in_dim(w_out, other, half, axis=1).astype(F32), 'tp', swap)
        wqkv_mine = lax.dynamic_slice_in_dim(w_qkv, mine, half, axis=0)
        wq_sib = lax.ppermute(lax.dynamic_slice_in_dim(w_query, other, half, axis=0).astype(F32), 'tp', swap)

        n, q, k, v, do = project(x, dout, gain, w_qkv, w_out, cos_t, sin_t)
        o, o32 = attn_fwd(q, k, v)
        o_sib = lax.ppermute(o32, 'tp', swap)
        block_out, dq, dq32, dkv32 = out_sum(chips, o, o_sib, wo_mine, wo_sib, x, q, k, v, do, cos_t, sin_t)
        dq_sib = lax.ppermute(dq32, 'tp', swap)
        dkv_sib = lax.ppermute(dkv32, 'tp', swap)
        gain_mine = lax.dynamic_slice_in_dim(gain, mine, half, axis=1)
        inner = w_query.shape[1]
        grad_hidden, gain_sum = grad_sum(chips, dq, dq_sib, dkv32, dkv_sib, wqkv_mine[:, :inner], wq_sib, wqkv_mine[:, inner:],
                                         x, dout, gain_mine)
        dkv = (dkv32 + dkv_sib).astype(BF16)
        grad_w_out = dot(o, dout, (0, 0))
        grad_w_query = dot(n, dq, (0, 0))
        grad_w_key = dot(n, dkv[:, :HEAD_DIM], (0, 0))
        grad_w_value = dot(n, dkv[:, HEAD_DIM:], (0, 0))
        return block_out[None], grad_hidden[None], gain_sum.reshape(-1), grad_w_query, grad_w_key, grad_w_value, grad_w_out

    act_spec = P('dp', None, None)
    return jax.shard_map(
        block_fn, mesh=mesh,
        in_specs=(act_spec, act_spec, P(None), P(None, 'tp'), P(None, None), P(None, None), P('tp', None)),
        out_specs=(act_spec, act_spec, P('dp'), P('dp', 'tp'), P('dp', 'tp'), P('dp', 'tp'), P(('dp', 'tp'), None)),
        check_vma=False)
```

```python
import functools
import math
import jax
import jax.numpy as jnp
import numpy as np
from jax import lax
from jax.experimental import pallas as pl
from jax.experimental.pallas import tpu as pltpu
from jax.sharding import PartitionSpec as P

HEAD_DIM = 128
NORM_EPS = 1.0e-5
ROPE_BASE = 10000.0
MASK_VALUE = -1.0e30
SCORE_SCALE = 1.0 / math.sqrt(HEAD_DIM)
EXP2_SCALE = SCORE_SCALE * math.log2(math.e)
ROWS = 256
WIDE = 512
BF16 = jnp.bfloat16
F32 = jnp.float32
VMEM_LIMIT = 66 * 10**6


def dot(a, b, contract):
    return lax.dot_general(a, b, ((contract[:1], contract[1:]), ((), ())), preferred_element_type=F32)


def rope_tables(count):
    def table(positions):
        inv_freq = ROPE_BASE ** (-np.arange(0, HEAD_DIM, 2, dtype=np.float64) / HEAD_DIM)
        angles = positions[:, None] * inv_freq[None, :]
        cos_t = np.repeat(np.cos(angles), 2, axis=1)
        sin_t = np.stack([-np.sin(angles), np.sin(angles)], axis=-1).reshape(cos_t.shape)
        return np.stack([cos_t, sin_t]).astype(np.float32)
    return table(np.arange(ROWS, dtype=np.float64)), table(ROWS * np.arange(count, dtype=np.float64))


def rope_block(b, low_ref, high_ref):
    cos_b, sin_b = high_ref[0, pl.ds(b, 1), :], high_ref[1, pl.ds(b, 1), :]
    cos_l, sin_l = low_ref[0], low_ref[1]
    return cos_b * cos_l - sin_b * sin_l, sin_b * cos_l + cos_b * sin_l


def rotate(t, cos_t, sin_t):
    even = lax.broadcasted_iota(jnp.int32, t.shape, 1) % 2 == 0
    swapped = jnp.where(even, pltpu.roll(t, HEAD_DIM - 1, 1), pltpu.roll(t, 1, 1))
    return t * cos_t + swapped * sin_t


def front_kernel(kv_ref, x_ref, gain_ref, wq_ref, wk_ref, wv_ref, low_ref, high_ref,
                 n_ref, q_ref, k_ref, v_ref, o_ref, wqkv, k_all, v_all):
    i = pl.program_id(0)
    seq = k_all.shape[0]

    @pl.when(i == 0)
    def _():
        k_all[...] = jnp.zeros_like(k_all)
        v_all[...] = jnp.zeros_like(v_all)
        wqkv[:, :2 * HEAD_DIM] = wq_ref[...]
        wqkv[:, 2 * HEAD_DIM:3 * HEAD_DIM] = wk_ref[...]
        wqkv[:, 3 * HEAD_DIM:] = wv_ref[...]

    x = x_ref[...].astype(F32)
    inv = lax.rsqrt(jnp.mean(x * x, axis=-1, keepdims=True) + NORM_EPS)
    n = (x * inv * gain_ref[...].astype(F32)).astype(BF16)
    n_ref[...] = n
    qkv = dot(n, wqkv[...], (1, 0))
    cos_t, sin_t = rope_block(i, low_ref, high_ref)
    q0 = rotate(qkv[:, :HEAD_DIM], cos_t, sin_t).astype(BF16)
    q1 = rotate(qkv[:, HEAD_DIM:2 * HEAD_DIM], cos_t, sin_t).astype(BF16)
    k = rotate(qkv[:, 2 * HEAD_DIM:3 * HEAD_DIM], cos_t, sin_t).astype(BF16)
    v = qkv[:, 3 * HEAD_DIM:].astype(BF16)
    q_ref[:, :HEAD_DIM] = q0
    q_ref[:, HEAD_DIM:] = q1
    k_ref[...] = k
    v_ref[...] = v
    rows = pl.ds(pl.multiple_of(i * ROWS, ROWS), ROWS)
    k_all[rows, :] = k
    v_all[rows, :] = v

    def attend(c):
        hi = (c + 1) * WIDE
        lo = hi - WIDE
        q2 = jnp.concatenate([q0, q1], axis=0)
        row_id = lax.broadcasted_iota(jnp.int32, (2 * ROWS, WIDE), 0) % ROWS + (i * ROWS - lo)
        causal = row_id >= lax.broadcasted_iota(jnp.int32, (2 * ROWS, WIDE), 1)
        s_diag = jnp.where(causal, dot(q2, k_all[lo:hi, :], (1, 1)), MASK_VALUE)
        m = jnp.max(s_diag, axis=-1, keepdims=True)
        if lo:
            s_pre = dot(q2, k_all[:lo, :], (1, 1))
            m = jnp.maximum(m, jnp.max(s_pre, axis=-1, keepdims=True))
        p_diag = jnp.exp2((s_diag - m) * EXP2_SCALE)
        total = jnp.sum(p_diag, axis=-1, keepdims=True)
        if lo:
            p_pre = jnp.exp2((s_pre - m) * EXP2_SCALE)
            total = total + jnp.sum(p_pre, axis=-1, keepdims=True)
        scale = 1.0 / total
        o2 = dot((p_diag * scale).astype(BF16), v_all[lo:hi, :], (1, 0))
        if lo:
            o2 = o2 + dot((p_pre * scale).astype(BF16), v_all[:lo, :], (1, 0))
        o_ref[:, :HEAD_DIM] = o2[:ROWS].astype(BF16)
        o_ref[:, HEAD_DIM:] = o2[ROWS:].astype(BF16)

    for c in range(seq // WIDE):
        pl.when(i // (WIDE // ROWS) == c)(lambda c=c: attend(c))


def front(kv_index, x, gain, wq, wk, wv, low, high):
    seq, d = x.shape
    row = lambda w: pl.BlockSpec((ROWS, w), lambda i, kv: (i, 0))
    whole = lambda a: pl.BlockSpec(a.shape, lambda i, kv: (0,) * a.ndim)
    head = pl.BlockSpec((d, HEAD_DIM), lambda i, kv: (0, kv[0]))
    widths = (d, 2 * HEAD_DIM, HEAD_DIM, HEAD_DIM, 2 * HEAD_DIM)
    return pl.pallas_call(
        front_kernel,
        grid_spec=pltpu.PrefetchScalarGridSpec(
            num_scalar_prefetch=1, grid=(seq // ROWS,),
            in_specs=[row(d), whole(gain), whole(wq), head, head, whole(low), whole(high)],
            out_specs=[row(w) for w in widths],
            scratch_shapes=[pltpu.VMEM((d, 4 * HEAD_DIM), BF16), pltpu.VMEM((seq, HEAD_DIM), BF16), pltpu.VMEM((seq, HEAD_DIM), BF16)]),
        out_shape=[jax.ShapeDtypeStruct((seq, w), BF16) for w in widths],
        compiler_params=pltpu.CompilerParams(vmem_limit_bytes=48 * 2**20),
        cost_estimate=pl.CostEstimate(flops=2 * seq * d * 4 * HEAD_DIM + 4 * seq * seq * HEAD_DIM, bytes_accessed=5 * seq * d, transcendentals=seq * seq),
        name='front')(kv_index, x, gain, wq, wk, wv, low, high)


def attn_bwd_rows(i, do_both, q_ref, k_ref, v_ref, low_ref, high_ref, dq32, dk_acc, dv_acc):
    lo, hi = i * ROWS, (i + 1) * ROWS
    rows = pl.ds(lo, ROWS)
    causal = lax.broadcasted_iota(jnp.int32, (ROWS, ROWS), 0) <= lax.broadcasted_iota(jnp.int32, (ROWS, ROWS), 1)
    dk_acc[lo:hi, :] = jnp.zeros((ROWS, HEAD_DIM), F32)
    dv_acc[lo:hi, :] = jnp.zeros((ROWS, HEAD_DIM), F32)

    def one_head(head, carry):
        cols = pl.ds(pl.multiple_of(head * HEAD_DIM, HEAD_DIM), HEAD_DIM)
        q, do = q_ref[rows, cols], do_both[:, cols]
        k_all, v_all = k_ref[:hi, :], v_ref[:hi, :]
        s_t = dot(k_all, q, (1, 1))
        s_diag = jnp.where(causal, s_t[lo:], MASK_VALUE)
        s_t = jnp.concatenate([s_t[:lo], s_diag], axis=0) if lo else s_diag
        m = jnp.max(s_t, axis=0, keepdims=True)
        p = jnp.exp2((s_t - m) * EXP2_SCALE)
        p = p * (1.0 / jnp.sum(p, axis=0, keepdims=True))
        dp = dot(v_all, do, (1, 1))
        delta = jnp.sum(p * dp, axis=0, keepdims=True)
        ds = (p * (dp - delta) * SCORE_SCALE).astype(BF16)
        dv_acc[:hi, :] += dot(p.astype(BF16), do, (1, 0))
        dk_acc[:hi, :] += dot(ds, q, (1, 0))
        dq = dot(ds, k_all, (0, 0))
        cos_t, sin_t = rope_block(i, low_ref, high_ref)
        dq32[rows, cols] = rotate(dq, cos_t, -sin_t).astype(BF16).astype(F32)
        return carry

    lax.fori_loop(0, 2, one_head, 0)


SUBS = 2


def ring_kernel_setup(n):
    me = lax.axis_index('tp')
    chip, core = me // 2, me % 2
    right = (chip + 1) % n * 2 + core
    left = (chip + n - 1) % n * 2 + core
    sib = me + 1 - 2 * core
    barrier = pltpu.get_barrier_semaphore()
    for peer in (right, left, sib):
        pl.semaphore_signal(barrier, inc=1, device_id={'tp': peer}, device_id_type=pl.DeviceIdType.MESH)
    pl.semaphore_wait(barrier, 3)
    return chip, core, right, left, sib


def remote(src, dst, send, recv, peer):
    return pltpu.make_async_remote_copy(src_ref=src, dst_ref=dst, send_sem=send, recv_sem=recv,
                                        device_id={'tp': peer}, device_id_type=pl.DeviceIdType.MESH)


def ring_sum(n, place, extra, partial, finish, rider, gather_rider, out_ref, gain_acc, bufs, sems):
    chip, core, right, left, sib = place
    rs_buf, ag_buf, sib_buf, obuf = bufs
    rs_send, rs_recv, ag_send, ag_recv, sib_send, sib_recv, out_sem, credit = sems
    width = rs_buf.shape[-1]
    block = out_ref.shape[0] // n
    sub_rows = block // SUBS
    half = 2 * width
    peers = (right, left)

    def part(slot_ref, sub, with_extra):
        return slot_ref.at[pl.ds(sub * sub_rows, sub_rows + (extra if with_extra and sub == SUBS - 1 else 0)), :]

    def rs_copy(s, sub, way):
        return remote(part(rs_buf.at[way, s], sub, False), part(rs_buf.at[way, s + 1], sub, False),
                      rs_send.at[way, s, sub], rs_recv.at[way, s, sub], peers[way])

    def ag_copy(s, sub, way):
        return remote(part(ag_buf.at[way, s], sub, True), part(ag_buf.at[way, s + 1], sub, True),
                      ag_send.at[way, s, sub], ag_recv.at[way, s, sub], peers[way])

    def sib_copy(s, sub, way):
        rows = sub_rows + (extra if sub == SUBS - 1 else 0)
        k = SUBS * s + sub
        return remote(part(ag_buf.at[way, s], sub, True), sib_buf.at[way, k % 4, pl.ds(0, rows), :],
                      sib_send.at[way, k], sib_recv.at[way, k], sib)

    def my_part(dest, sub, way):
        row = pl.multiple_of(dest * block + sub * sub_rows, sub_rows)
        return partial(pl.ds(row, sub_rows), way)

    def dest_of(s, way):
        return (chip + n - 1 - s) % n if way == 0 else (chip + 1 + s) % n

    def local(ref, sub):
        return pl.ds(sub * sub_rows, sub_rows)

    for sub in range(SUBS):
        for way in range(2):
            rs_buf[way, 0, local(rs_buf, sub), :] = my_part(dest_of(0, way), sub, way)
            rs_copy(0, sub, way).start()
    rider(0)

    def rs_step(s, carry):
        for sub in range(SUBS):
            for way in range(2):
                rs_copy(s - 1, sub, way).wait_recv()
                rs_buf[way, s, local(rs_buf, sub), :] += my_part(dest_of(s, way), sub, way)
                rs_copy(s, sub, way).start()
            if sub == 0:
                rider(s)
        return carry

    lax.fori_loop(1, n - 1, rs_step, 0)
    for sub in range(SUBS):
        for way in range(2):
            rs_copy(n - 2, sub, way).wait_recv()
        finish(sub, [rs_buf[way, n - 1, local(rs_buf, sub), :] + my_part(chip, sub, way) for way in range(2)])

    def out_copy(whose, s, sub, way):
        b = (chip + n - s) % n if way == 0 else (chip + s) % n
        col = (core if whose == 0 else 1 - core) * half + way * width
        dst = out_ref.at[pl.ds(pl.multiple_of(b * block + sub * sub_rows, sub_rows), sub_rows), pl.ds(pl.multiple_of(col, 128), width)]
        return pltpu.make_async_copy(obuf.at[whose, sub, way], dst, out_sem.at[whose, sub, way])

    def emit(whose, s, sub, way, values):
        @pl.when(s >= 1)
        def _():
            out_copy(whose, s - 1, sub, way).wait()
        obuf[whose, sub, way] = values.astype(BF16)
        out_copy(whose, s, sub, way).start()

    def own_chunk(s, sub, forward):
        @pl.when(s >= 2)
        def _():
            pl.semaphore_wait(credit, 1)
        for way in range(2):
            if forward:
                ag_copy(s, sub, way).start()
            sib_copy(s, sub, way).start()
        for way in range(2):
            emit(0, s, sub, way, ag_buf[way, s, local(ag_buf, sub), :])
            if extra and sub == SUBS - 1:
                gain_acc[0, way] += ag_buf[way, s, pl.ds(block, extra), :]

    def sib_chunk(s, sub):
        k = SUBS * s + sub
        for way in range(2):
            sib_copy(s, sub, way).wait_recv()
            emit(1, s, sub, way, sib_buf[way, k % 4, pl.ds(0, sub_rows), :])
            if extra and sub == SUBS - 1:
                gain_acc[1, way] += sib_buf[way, k % 4, pl.ds(sub_rows, extra), :]

        @pl.when(s < n - 2)
        def _():
            pl.semaphore_signal(credit, inc=1, device_id={'tp': sib}, device_id_type=pl.DeviceIdType.MESH)

    own_chunk(0, 0, True)
    own_chunk(0, 1, True)
    rider(n - 1)
    sib_chunk(0, 0)

    def ag_step(s, carry):
        for sub in range(SUBS):
            for way in range(2):
                ag_copy(s - 1, sub, way).wait_recv()
            own_chunk(s, sub, True)
            if sub == 0:
                sib_chunk(s - 1, 1)
                gather_rider(s)
            else:
                sib_chunk(s, 0)
        return carry

    lax.fori_loop(1, n - 1, ag_step, 0)
    last = n - 1
    for sub in range(SUBS):
        for way in range(2):
            ag_copy(last - 1, sub, way).wait_recv()
        own_chunk(last, sub, False)
        if sub == 0:
            sib_chunk(last - 1, 1)
        else:
            sib_chunk(last, 0)
    sib_chunk(last, 1)
    for sub in range(SUBS):
        for way in range(2):
            for whose in range(2):
                out_copy(whose, last, sub, way).wait()

    def drain(s, carry):
        for sub in range(SUBS):
            for way in range(2):
                rs_copy(s, sub, way).wait_send()
                ag_copy(s, sub, way).wait_send()
                sib_copy(s, sub, way).wait_send()
        return carry

    lax.fori_loop(0, n - 1, drain, 0)
    for sub in range(SUBS):
        for way in range(2):
            sib_copy(last, sub, way).wait_send()


def ring_scratch(n, seq, d_model, extra):
    width, block = d_model // 4, seq // n
    sub_rows = block // SUBS
    dma = pltpu.SemaphoreType.DMA
    return [
        pltpu.VMEM((2, n, block, width), F32),
        pltpu.VMEM((2, n, block + extra, width), F32),
        pltpu.VMEM((2, 4, sub_rows + extra, width), F32),
        pltpu.VMEM((2, SUBS, 2, sub_rows, width), BF16),
        dma((2, n - 1, SUBS)), dma((2, n - 1, SUBS)), dma((2, n - 1, SUBS)), dma((2, n - 1, SUBS)),
        dma((2, SUBS * n)), dma((2, SUBS * n)), dma((2, SUBS, 2)), pltpu.SemaphoreType.REGULAR,
    ]


def out_kernel(n, o_ref, wo_ref, q_ref, k_ref, v_ref, low_ref, high_ref, x_ref, dout_ref,
               out_ref, dlhs_ref, lhs, rhs, x_rows, dout_rows, do_blk, dk_acc, x32, dkv32, wo32, o_got, wo_got, dq_got, dkv_got,
               row_sem, dout_sem, swap_send, swap_recv, *ring):
    bufs, sems = ring[:4], ring[4:]
    place = ring_kernel_setup(n)
    chip, core, right, left, sib = place
    width = bufs[0].shape[-1]
    half = 2 * width
    block = x_rows.shape[0]
    inner = o_ref.shape[1]
    count = q_ref.shape[0] // ROWS
    x_copy = pltpu.make_async_copy(
        x_ref.at[pl.ds(pl.multiple_of(chip * block, block), block), pl.ds(pl.multiple_of(core * half, 128), half)],
        x_rows, row_sem)

    def dout_copy(i):
        return pltpu.make_async_copy(dout_ref.at[pl.ds(i * ROWS, ROWS), :], dout_rows.at[i % 2], dout_sem.at[i % 2])

    swaps = [remote(src, dst, swap_send.at[k], swap_recv.at[k], sib)
             for k, (src, dst) in enumerate([(wo32, wo_got), (x32, o_got), (x32, dq_got), (dkv32, dkv_got)])]
    wo32[...] = wo_ref[:, pl.ds(pl.multiple_of((1 - core) * half, 128), half)].astype(F32)
    swaps[0].start()
    x32[...] = o_ref[...].astype(F32)
    swaps[1].start()
    x_copy.start()
    dout_copy(0).start()
    lhs[:, :inner] = o_ref[...]
    rhs[:inner, :] = wo_ref[:, pl.ds(pl.multiple_of(core * half, 128), half)]
    swaps[0].wait()
    rhs[inner:, :] = wo_got[...].astype(BF16)
    swaps[1].wait()
    lhs[:, inner:] = o_got[...].astype(BF16)

    def partial(rows, way):
        return dot(lhs[rows, :], rhs[:, way * width:(way + 1) * width], (1, 0))

    sub_rows = block // SUBS

    def finish(sub, sums):
        if sub == 0:
            x_copy.wait()
        for way in range(2):
            rows = pl.ds(sub * sub_rows, sub_rows)
            bufs[1][way, 0, rows, :] = sums[way] + x_rows[rows, way * width:(way + 1) * width].astype(F32)

    dv_acc = dkv32.at[:, pl.ds(HEAD_DIM, HEAD_DIM)]

    def ride(step):
        for i in range(step * count // n, (step + 1) * count // n):
            dout_copy(i).wait()
            if i + 1 < count:
                dout_copy(i + 1).start()
            do_blk[...] = dot(dout_rows[i % 2], wo_ref[...], (1, 1)).astype(BF16)
            attn_bwd_rows(i, do_blk, q_ref, k_ref, v_ref, low_ref, high_ref, x32, dk_acc, dv_acc)
        if step == n - 1:
            def turn_back(b, carry):
                rows = pl.ds(pl.multiple_of(b * ROWS, ROWS), ROWS)
                cos_t, sin_t = rope_block(b, low_ref, high_ref)
                dkv32[rows, :HEAD_DIM] = rotate(dk_acc[rows, :], cos_t, -sin_t)
                return carry
            lax.fori_loop(0, count, turn_back, 0)
            swaps[2].start()
            swaps[3].start()

    def rider(step):
        if isinstance(step, int):
            ride(step)
        else:
            for static in range(1, n - 1):
                pl.when(step == static)(lambda static=static: ride(static))

    def gather_rider(step):
        @pl.when(step == n // 2)
        def _():
            swaps[2].wait()
            swaps[3].wait()
            dlhs_ref[:, :inner] = x32[...].astype(BF16)
            dlhs_ref[:, inner:2 * inner] = (dkv32[...] + dkv_got[...]).astype(BF16)
            dlhs_ref[:, 2 * inner:] = dq_got[...].astype(BF16)

    ring_sum(n, place, 0, partial, finish, rider, gather_rider, out_ref, None, bufs, sems)


def grad_kernel(n, lhs, wqsib_ref, gain_ref, wq_ref, wk_ref, wv_ref, x_ref, dout_ref,
                out_ref, gsum_ref, rhs, gain, x_rows, dout_rows, unit_buf, stat_buf, gain_acc, row_sem, stat_send, stat_recv, *ring):
    bufs, sems = ring[:4], ring[4:]
    place = ring_kernel_setup(n)
    chip, core, right, left, sib = place
    width = bufs[0].shape[-1]
    block = x_rows.shape[0]
    inner = wq_ref.shape[1]
    half = 2 * width
    row = pl.multiple_of(chip * block, block)
    col = pl.multiple_of(core * half, 128)
    head_cols = pl.ds(pl.multiple_of(chip * HEAD_DIM, HEAD_DIM), HEAD_DIM)
    x_copy = pltpu.make_async_copy(x_ref.at[pl.ds(row, block), :], x_rows, row_sem.at[0])
    dout_copy = pltpu.make_async_copy(dout_ref.at[pl.ds(row, block), pl.ds(col, half)], dout_rows, row_sem.at[1])
    weights = [
        pltpu.make_async_copy(wq_ref.at[pl.ds(col, half), :], rhs.at[:, pl.ds(0, inner)], row_sem.at[2]),
        pltpu.make_async_copy(wk_ref.at[pl.ds(col, half), head_cols], rhs.at[:, pl.ds(inner, HEAD_DIM)], row_sem.at[3]),
        pltpu.make_async_copy(wv_ref.at[pl.ds(col, half), head_cols], rhs.at[:, pl.ds(inner + HEAD_DIM, HEAD_DIM)], row_sem.at[4]),
    ]
    for copy in weights + [x_copy, dout_copy]:
        copy.start()
    rhs[:, inner + 2 * HEAD_DIM:] = wqsib_ref[...].astype(BF16)
    gain[...] = gain_ref[:, pl.ds(col, half)].astype(F32)
    for copy in weights:
        copy.wait()
    gain_acc[...] = jnp.zeros_like(gain_acc)

    def partial(rows, way):
        return dot(lhs[rows, :], rhs[way * width:(way + 1) * width, :], (1, 1))

    sub_rows = block // SUBS

    def prepare(sub):
        rows = pl.ds(sub * sub_rows, sub_rows)
        x = x_rows[rows, :].astype(F32)
        inv = lax.rsqrt(jnp.mean(x * x, axis=-1, keepdims=True) + NORM_EPS)
        stat_buf[2, rows, :] = jnp.broadcast_to(inv, (sub_rows, HEAD_DIM))
        mine = x_rows[rows, pl.ds(col, half)].astype(F32)
        unit_buf[rows, :] = mine * inv

    def rider(step):
        if isinstance(step, int) and step == 0:
            x_copy.wait()
            dout_copy.wait()
            for sub in range(SUBS):
                prepare(sub)

    def stat_copy(sub):
        rows = pl.ds(sub * sub_rows, sub_rows)
        return remote(stat_buf.at[0, rows, :], stat_buf.at[1, rows, :], stat_send.at[sub], stat_recv.at[sub], sib)

    def finish(sub, sums):
        rows = pl.ds(sub * sub_rows, sub_rows)
        ag_buf = bufs[1]
        total = jnp.zeros((sub_rows, 1), F32)
        for way in range(2):
            cols = slice(way * width, (way + 1) * width)
            unit = unit_buf[rows, cols]
            prod = sums[way] * unit
            total = total + jnp.sum(prod * gain[:, cols], axis=-1, keepdims=True)
            gsum = jnp.sum(prod.reshape(sub_rows // 8, 8, width), axis=0)
            ag_buf[way, 0, pl.ds(block, 8), :] = gsum if sub == 0 else gsum + ag_buf[way, 0, pl.ds(block, 8), :]
            ag_buf[way, 0, rows, :] = sums[way]
        stat_buf[0, rows, :] = jnp.broadcast_to(total, (sub_rows, HEAD_DIM))
        stat_copy(sub).start()
        stat_copy(sub).wait()
        mean = (stat_buf[0, rows, 0:1] + stat_buf[1, rows, 0:1]) * (1.0 / (2 * half))
        inv = stat_buf[2, rows, 0:1]
        for way in range(2):
            cols = slice(way * width, (way + 1) * width)
            scaled = ag_buf[way, 0, rows, :] * gain[:, cols]
            ag_buf[way, 0, rows, :] = dout_rows[rows, cols].astype(F32) + inv * (scaled - unit_buf[rows, cols] * mean)

    ring_sum(n, place, 8, partial, finish, rider, lambda step: None, out_ref, gain_acc, bufs, sems)
    for way in range(2):
        gsum_ref[core, way] = jnp.sum(gain_acc[0, way], axis=0, keepdims=True)
        gsum_ref[1 - core, way] = jnp.sum(gain_acc[1, way], axis=0, keepdims=True)


def final_kernel(n_ref, dout_ref, o_ref, d_ref, out_in, gh_in, out_ref, gh_ref, wq_ref, wk_ref, wv_ref, wo_ref):
    inner = o_ref.shape[1]
    out_ref[...] = out_in[...]
    gh_ref[...] = gh_in[...]
    dw = dot(n_ref[...], d_ref[:, :2 * inner], (0, 0))
    wq_ref[...] = dw[:, :inner]
    wk_ref[...] = dw[:, inner:inner + HEAD_DIM]
    wv_ref[...] = dw[:, inner + HEAD_DIM:]
    wo_ref[...] = dot(o_ref[...], dout_ref[...], (0, 0))


def final(n, dout, o, dlhs, out, gh):
    seq, d = n.shape
    inner = o.shape[1]
    col = pl.BlockSpec((seq, ROWS), lambda j: (0, j))
    whole = lambda a: pl.BlockSpec(a.shape, lambda j: (0, 0))
    row = lambda w: pl.BlockSpec((ROWS, w), lambda j: (j, 0))
    shape = jax.ShapeDtypeStruct
    return pl.pallas_call(
        final_kernel, grid=(d // ROWS,),
        in_specs=[col, col, whole(o), whole(dlhs), col, col],
        out_specs=[col, col, row(inner), row(HEAD_DIM), row(HEAD_DIM), pl.BlockSpec((inner, ROWS), lambda j: (0, j))],
        out_shape=[shape(out.shape, BF16), shape(gh.shape, BF16), shape((d, inner), F32), shape((d, HEAD_DIM), F32),
                   shape((d, HEAD_DIM), F32), shape((inner, d), F32)],
        compiler_params=pltpu.CompilerParams(vmem_limit_bytes=48 * 2**20),
        cost_estimate=pl.CostEstimate(flops=6 * seq * inner * d, bytes_accessed=14 * seq * d, transcendentals=0),
        name='final')(n, dout, o, dlhs, out, gh)


def out_sum(n, o, wo, q, k, v, low, high, x, dout):
    seq, d_model = x.shape
    half, block, inner = d_model // 2, seq // n, o.shape[1]
    vmem, hbm = pl.BlockSpec(memory_space=pltpu.VMEM), pl.BlockSpec(memory_space=pl.ANY)
    shape = jax.ShapeDtypeStruct
    dma = pltpu.SemaphoreType.DMA
    rows32 = pltpu.VMEM((seq, inner), F32)
    wide32 = pltpu.VMEM((inner, half), F32)
    return pl.pallas_call(
        functools.partial(out_kernel, n),
        out_shape=[shape((seq, d_model), BF16), shape((seq, 2 * inner + 2 * HEAD_DIM), BF16)],
        in_specs=[vmem] * 7 + [hbm] * 2, out_specs=[hbm, vmem],
        scratch_shapes=[pltpu.VMEM((seq, 2 * inner), BF16), pltpu.VMEM((2 * inner, half), BF16),
                        pltpu.VMEM((block, half), BF16), pltpu.VMEM((2, ROWS, d_model), BF16), pltpu.VMEM((ROWS, inner), BF16),
                        pltpu.VMEM((seq, HEAD_DIM), F32), rows32, rows32, wide32, rows32, wide32, rows32, rows32,
                        dma, dma((2,)), dma((4,)), dma((4,))]
        + ring_scratch(n, seq, d_model, 0),
        compiler_params=pltpu.CompilerParams(collective_id=1, has_side_effects=True, vmem_limit_bytes=VMEM_LIMIT),
        cost_estimate=pl.CostEstimate(flops=10 * seq * seq * HEAD_DIM, bytes_accessed=4 * seq * d_model, transcendentals=seq * seq),
        name='out_sum')(o, wo, q, k, v, low, high, x, dout)


def grad_sum(n, dlhs, wq_sib, gain, wq, wk, wv, x, dout):
    seq, d_model = x.shape
    half, block, width = d_model // 2, seq // n, d_model // 4
    kdim = dlhs.shape[1]
    vmem, hbm = pl.BlockSpec(memory_space=pltpu.VMEM), pl.BlockSpec(memory_space=pl.ANY)
    shape = jax.ShapeDtypeStruct
    dma = pltpu.SemaphoreType.DMA
    return pl.pallas_call(
        functools.partial(grad_kernel, n),
        out_shape=[shape((seq, d_model), BF16), shape((2, 2, 1, width), F32)],
        in_specs=[vmem] * 3 + [hbm] * 5, out_specs=[hbm, vmem],
        scratch_shapes=[pltpu.VMEM((half, kdim), BF16), pltpu.VMEM((1, half), F32),
                        pltpu.VMEM((block, d_model), BF16), pltpu.VMEM((block, half), BF16), pltpu.VMEM((block, half), F32),
                        pltpu.VMEM((3, block, HEAD_DIM), F32), pltpu.VMEM((2, 2, 8, width), F32),
                        dma((5,)), dma((SUBS,)), dma((SUBS,))]
        + ring_scratch(n, seq, d_model, 8),
        compiler_params=pltpu.CompilerParams(collective_id=2, has_side_effects=True, vmem_limit_bytes=VMEM_LIMIT),
        cost_estimate=pl.CostEstimate(flops=4 * seq * kdim * half, bytes_accessed=4 * seq * d_model, transcendentals=0),
        name='grad_sum')(dlhs, wq_sib, gain, wq, wk, wv, x, dout)


def solution(mesh):
    tp_size = mesh.shape['tp']
    chips = tp_size // 2
    swap = [(source, source ^ 1) for source in range(tp_size)]

    def block_fn(hidden, grad_out, norm_gain, w_query, w_key, w_value, w_out):
        batch, seq_len, d_model = hidden.shape
        half = d_model // 2
        tp_index = lax.axis_index('tp')
        kv_index, core = tp_index // 2, tp_index % 2
        low, high = rope_tables(seq_len // ROWS)
        x, dout = hidden[0], grad_out[0]
        gain = norm_gain[None, :]
        wq_sib = lax.ppermute(lax.dynamic_slice_in_dim(w_query, (1 - core) * half, half, axis=0).astype(F32), 'tp', swap)
        n, q, k, v, o = front(kv_index[None], x, gain, w_query, w_key, w_value, low, high)
        out, dlhs = out_sum(chips, o, w_out, q, k, v, low, high, x, dout)
        gh, gain_sum = grad_sum(chips, dlhs, wq_sib, gain, w_query, w_key, w_value, x, dout)
        out, gh, grad_w_query, grad_w_key, grad_w_value, grad_w_out = final(n, dout, o, dlhs, out, gh)
        return out[None], gh[None], gain_sum.reshape(-1), grad_w_query, grad_w_key, grad_w_value, grad_w_out

    act_spec = P('dp', None, None)
    return jax.shard_map(
        block_fn, mesh=mesh,
        in_specs=(act_spec, act_spec, P(None), P(None, 'tp'), P(None, None), P(None, None), P('tp', None)),
        out_specs=(act_spec, act_spec, P('dp'), P('dp', 'tp'), P('dp', 'tp'), P('dp', 'tp'), P(('dp', 'tp'), None)),
        check_vma=False)
```

```python
import functools
import math
import jax
import jax.numpy as jnp
import numpy as np
from jax import lax
from jax.experimental import pallas as pl
from jax.experimental.pallas import tpu as pltpu
from jax.sharding import PartitionSpec as P

HEAD_DIM = 128
NORM_EPS = 1.0e-5
ROPE_BASE = 10000.0
MASK_VALUE = -1.0e30
SCORE_SCALE = 1.0 / math.sqrt(HEAD_DIM)
EXP2_SCALE = SCORE_SCALE * math.log2(math.e)
ROWS = 256
WIDE = 512
BF16 = jnp.bfloat16
F32 = jnp.float32
VMEM_LIMIT = 66 * 10**6


def dot(a, b, contract):
    return lax.dot_general(a, b, ((contract[:1], contract[1:]), ((), ())), preferred_element_type=F32)


def rope_tables(count):
    def table(positions):
        inv_freq = ROPE_BASE ** (-np.arange(0, HEAD_DIM, 2, dtype=np.float64) / HEAD_DIM)
        angles = positions[:, None] * inv_freq[None, :]
        cos_t = np.repeat(np.cos(angles), 2, axis=1)
        sin_t = np.stack([-np.sin(angles), np.sin(angles)], axis=-1).reshape(cos_t.shape)
        return np.stack([cos_t, sin_t]).astype(np.float32)
    return table(np.arange(ROWS, dtype=np.float64)), table(ROWS * np.arange(count, dtype=np.float64))


def rope_block(b, low_ref, high_ref):
    cos_b, sin_b = high_ref[0, pl.ds(b, 1), :], high_ref[1, pl.ds(b, 1), :]
    cos_l, sin_l = low_ref[0], low_ref[1]
    return cos_b * cos_l - sin_b * sin_l, sin_b * cos_l + cos_b * sin_l


def rotate(t, cos_t, sin_t):
    even = lax.broadcasted_iota(jnp.int32, t.shape, 1) % 2 == 0
    swapped = jnp.where(even, pltpu.roll(t, HEAD_DIM - 1, 1), pltpu.roll(t, 1, 1))
    return t * cos_t + swapped * sin_t


def front_kernel(kv_ref, x_ref, gain_ref, wq_ref, wk_ref, wv_ref, low_ref, high_ref,
                 n_ref, q_ref, k_ref, v_ref, o_ref, wq32_ref, wqkv, k_all, v_all):
    i = pl.program_id(0)
    seq = k_all.shape[0]
    half = wq32_ref.shape[0]

    @pl.when(i == 0)
    def _():
        wqkv[:, :2 * HEAD_DIM] = wq_ref[...]
        wqkv[:, 2 * HEAD_DIM:3 * HEAD_DIM] = wk_ref[...]
        wqkv[:, 3 * HEAD_DIM:] = wv_ref[...]
        wq32_ref[...] = wq_ref[pl.ds(pl.multiple_of(kv_ref[1] * half, half), half), :].astype(F32)

    parts = []
    for r in range(0, WIDE, ROWS):
        rows = slice(r, r + ROWS)
        x = x_ref[rows, :].astype(F32)
        inv = lax.rsqrt(jnp.mean(x * x, axis=-1, keepdims=True) + NORM_EPS)
        n_ref[rows, :] = (x * inv * gain_ref[...].astype(F32)).astype(BF16)
        parts.append(rope_block(i * (WIDE // ROWS) + r // ROWS, low_ref, high_ref))
    qkv = dot(n_ref[...], wqkv[...], (1, 0))
    cos_t, sin_t = (jnp.concatenate([p[t] for p in parts], axis=0) for t in range(2))
    q0 = rotate(qkv[:, :HEAD_DIM], cos_t, sin_t).astype(BF16)
    q1 = rotate(qkv[:, HEAD_DIM:2 * HEAD_DIM], cos_t, sin_t).astype(BF16)
    k = rotate(qkv[:, 2 * HEAD_DIM:3 * HEAD_DIM], cos_t, sin_t).astype(BF16)
    v = qkv[:, 3 * HEAD_DIM:].astype(BF16)
    q_ref[:, :HEAD_DIM] = q0
    q_ref[:, HEAD_DIM:] = q1
    k_ref[...] = k
    v_ref[...] = v
    rows = pl.ds(pl.multiple_of(i * WIDE, WIDE), WIDE)
    k_all[rows, :] = k
    v_all[rows, :] = v

    def attend(c):
        lo, hi = c * WIDE, (c + 1) * WIDE
        q2 = jnp.concatenate([q0, q1], axis=0)
        row_id = lax.broadcasted_iota(jnp.int32, (2 * WIDE, WIDE), 0) % WIDE
        causal = row_id >= lax.broadcasted_iota(jnp.int32, (2 * WIDE, WIDE), 1)
        s_diag = jnp.where(causal, dot(q2, k_all[lo:hi, :], (1, 1)), MASK_VALUE)
        m = jnp.max(s_diag, axis=-1, keepdims=True)
        if lo:
            s_pre = dot(q2, k_all[:lo, :], (1, 1))
            m = jnp.maximum(m, jnp.max(s_pre, axis=-1, keepdims=True))
        p_diag = jnp.exp2((s_diag - m) * EXP2_SCALE)
        total = jnp.sum(p_diag, axis=-1, keepdims=True)
        if lo:
            p_pre = jnp.exp2((s_pre - m) * EXP2_SCALE)
            total = total + jnp.sum(p_pre, axis=-1, keepdims=True)
        scale = 1.0 / total
        o2 = dot((p_diag * scale).astype(BF16), v_all[lo:hi, :], (1, 0))
        if lo:
            o2 = o2 + dot((p_pre * scale).astype(BF16), v_all[:lo, :], (1, 0))
        o_ref[:, :HEAD_DIM] = o2[:WIDE].astype(BF16)
        o_ref[:, HEAD_DIM:] = o2[WIDE:].astype(BF16)

    for c in range(seq // WIDE):
        pl.when(i == c)(lambda c=c: attend(c))


def front(scalars, x, gain, wq, wk, wv, low, high):
    seq, d = x.shape
    row = lambda w: pl.BlockSpec((WIDE, w), lambda i, kv: (i, 0))
    whole = lambda shape: pl.BlockSpec(shape, lambda i, kv: (0,) * len(shape))
    head = pl.BlockSpec((d, HEAD_DIM), lambda i, kv: (0, kv[0]))
    widths = (d, 2 * HEAD_DIM, HEAD_DIM, HEAD_DIM, 2 * HEAD_DIM)
    return pl.pallas_call(
        front_kernel,
        grid_spec=pltpu.PrefetchScalarGridSpec(
            num_scalar_prefetch=1, grid=(seq // WIDE,),
            in_specs=[row(d), whole(gain.shape), whole(wq.shape), head, head, whole(low.shape), whole(high.shape)],
            out_specs=[row(w) for w in widths] + [whole((d // 2, wq.shape[1]))],
            scratch_shapes=[pltpu.VMEM((d, 4 * HEAD_DIM), BF16), pltpu.VMEM((seq, HEAD_DIM), BF16), pltpu.VMEM((seq, HEAD_DIM), BF16)]),
        out_shape=[jax.ShapeDtypeStruct((seq, w), BF16) for w in widths] + [jax.ShapeDtypeStruct((d // 2, wq.shape[1]), F32)],
        compiler_params=pltpu.CompilerParams(vmem_limit_bytes=VMEM_LIMIT),
        cost_estimate=pl.CostEstimate(flops=2 * seq * d * 4 * HEAD_DIM + 4 * seq * seq * HEAD_DIM, bytes_accessed=5 * seq * d, transcendentals=seq * seq),
        name='front')(scalars, x, gain, wq, wk, wv, low, high)


def attn_bwd_rows(i, do_both, q_ref, k_ref, v_ref, low_ref, high_ref, dq32, dk_acc, dv_acc):
    lo, hi = i * ROWS, (i + 1) * ROWS
    rows = pl.ds(lo, ROWS)
    causal = lax.broadcasted_iota(jnp.int32, (ROWS, ROWS), 0) <= lax.broadcasted_iota(jnp.int32, (ROWS, ROWS), 1)
    dk_acc[lo:hi, :] = jnp.zeros((ROWS, HEAD_DIM), F32)
    dv_acc[lo:hi, :] = jnp.zeros((ROWS, HEAD_DIM), F32)

    def one_head(head, carry):
        cols = pl.ds(pl.multiple_of(head * HEAD_DIM, HEAD_DIM), HEAD_DIM)
        q, do = q_ref[rows, cols], do_both[:, cols]
        k_all, v_all = k_ref[:hi, :], v_ref[:hi, :]
        s_t = dot(k_all, q, (1, 1))
        s_diag = jnp.where(causal, s_t[lo:], MASK_VALUE)
        s_t = jnp.concatenate([s_t[:lo], s_diag], axis=0) if lo else s_diag
        m = jnp.max(s_t, axis=0, keepdims=True)
        p = jnp.exp2((s_t - m) * EXP2_SCALE)
        p = p * (1.0 / jnp.sum(p, axis=0, keepdims=True))
        dp = dot(v_all, do, (1, 1))
        delta = jnp.sum(p * dp, axis=0, keepdims=True)
        ds = (p * (dp - delta) * SCORE_SCALE).astype(BF16)
        dv_acc[:hi, :] += dot(p.astype(BF16), do, (1, 0))
        dk_acc[:hi, :] += dot(ds, q, (1, 0))
        dq = dot(ds, k_all, (0, 0))
        cos_t, sin_t = rope_block(i, low_ref, high_ref)
        dq32[rows, cols] = rotate(dq, cos_t, -sin_t).astype(BF16).astype(F32)
        return carry

    lax.fori_loop(0, 2, one_head, 0)


SUBS = 4


def ring_kernel_setup(n):
    me = lax.axis_index('tp')
    chip, core = me // 2, me % 2
    right = (chip + 1) % n * 2 + core
    left = (chip + n - 1) % n * 2 + core
    sib = me + 1 - 2 * core
    barrier = pltpu.get_barrier_semaphore()
    for peer in (right, left, sib):
        pl.semaphore_signal(barrier, inc=1, device_id={'tp': peer}, device_id_type=pl.DeviceIdType.MESH)
    return chip, core, right, left, sib


def peers_ready():
    pl.semaphore_wait(pltpu.get_barrier_semaphore(), 3)


def remote(src, dst, send, recv, peer):
    return pltpu.make_async_remote_copy(src_ref=src, dst_ref=dst, send_sem=send, recv_sem=recv,
                                        device_id={'tp': peer}, device_id_type=pl.DeviceIdType.MESH)


def ring_sum(n, place, extra, partial, finish, rider, gather_rider, out_ref, gain_acc, bufs, sems):
    chip, core, right, left, sib = place
    rs_buf, ag_buf, sib_buf, obuf = bufs
    rs_send, rs_recv, ag_send, ag_recv, sib_send, sib_recv, out_sem, credit = sems
    width = rs_buf.shape[-1]
    block = out_ref.shape[0] // n
    sub_rows = block // SUBS
    half = 2 * width
    peers = (right, left)

    def part(slot_ref, sub, with_extra):
        return slot_ref.at[pl.ds(sub * sub_rows, sub_rows + (extra if with_extra and sub == SUBS - 1 else 0)), :]

    def rs_copy(s, sub, way):
        return remote(part(rs_buf.at[way, s], sub, False), part(rs_buf.at[way, s + 1], sub, False),
                      rs_send.at[way, s, sub], rs_recv.at[way, s, sub], peers[way])

    def ag_copy(s, sub, way):
        return remote(part(ag_buf.at[way, s], sub, True), part(ag_buf.at[way, s + 1], sub, True),
                      ag_send.at[way, s, sub], ag_recv.at[way, s, sub], peers[way])

    def sib_copy(s, sub, way):
        rows = sub_rows + (extra if sub == SUBS - 1 else 0)
        k = SUBS * s + sub
        return remote(part(ag_buf.at[way, s], sub, True), sib_buf.at[way, k % (2 * SUBS), pl.ds(0, rows), :],
                      sib_send.at[way, k], sib_recv.at[way, k], sib)

    def my_part(dest, sub, way):
        row = pl.multiple_of(dest * block + sub * sub_rows, sub_rows)
        return partial(pl.ds(row, sub_rows), way)

    def dest_of(s, way):
        return (chip + n - 1 - s) % n if way == 0 else (chip + 1 + s) % n

    def local(ref, sub):
        return pl.ds(sub * sub_rows, sub_rows)

    for sub in range(SUBS):
        for way in range(2):
            rs_buf[way, 0, local(rs_buf, sub), :] = my_part(dest_of(0, way), sub, way)
            rs_copy(0, sub, way).start()
    rider(0)

    def rs_step(s, carry):
        for sub in range(SUBS):
            for way in range(2):
                term = my_part(dest_of(s, way), sub, way)
                rs_copy(s - 1, sub, way).wait_recv()
                rs_buf[way, s, local(rs_buf, sub), :] += term
                rs_copy(s, sub, way).start()
            if sub == 0:
                rider(s)
        return carry

    lax.fori_loop(1, n - 1, rs_step, 0)

    def out_copy(whose, s, sub, way):
        b = (chip + n - s) % n if way == 0 else (chip + s) % n
        col = (core if whose == 0 else 1 - core) * half + way * width
        dst = out_ref.at[pl.ds(pl.multiple_of(b * block + sub * sub_rows, sub_rows), sub_rows), pl.ds(pl.multiple_of(col, 128), width)]
        return pltpu.make_async_copy(obuf.at[whose, sub, way], dst, out_sem.at[whose, sub, way])

    def emit(whose, s, sub, way, values):
        @pl.when(s >= 1)
        def _():
            out_copy(whose, s - 1, sub, way).wait()
        obuf[whose, sub, way] = values.astype(BF16)
        out_copy(whose, s, sub, way).start()

    def own_chunk(s, sub, forward):
        @pl.when(s >= 2)
        def _():
            pl.semaphore_wait(credit, 1)
        for way in range(2):
            if forward:
                ag_copy(s, sub, way).start()
            sib_copy(s, sub, way).start()
        for way in range(2):
            emit(0, s, sub, way, ag_buf[way, s, local(ag_buf, sub), :])
            if extra and sub == SUBS - 1:
                gain_acc[0, way] += ag_buf[way, s, pl.ds(block, extra), :]

    def sib_chunk(s, sub):
        k = SUBS * s + sub
        for way in range(2):
            sib_copy(s, sub, way).wait_recv()
            emit(1, s, sub, way, sib_buf[way, k % (2 * SUBS), pl.ds(0, sub_rows), :])
            if extra and sub == SUBS - 1:
                gain_acc[1, way] += sib_buf[way, k % (2 * SUBS), pl.ds(sub_rows, extra), :]

        @pl.when(s < n - 2)
        def _():
            pl.semaphore_signal(credit, inc=1, device_id={'tp': sib}, device_id_type=pl.DeviceIdType.MESH)

    for sub in range(SUBS):
        terms = [my_part(chip, sub, way) for way in range(2)]
        for way in range(2):
            rs_copy(n - 2, sub, way).wait_recv()
        finish(sub, [rs_buf[way, n - 1, local(rs_buf, sub), :] + terms[way] for way in range(2)])
        own_chunk(0, sub, True)
        if sub:
            sib_chunk(0, sub - 1)
    rider(n - 1)

    def ag_step(s, carry):
        for sub in range(SUBS):
            for way in range(2):
                ag_copy(s - 1, sub, way).wait_recv()
            own_chunk(s, sub, True)
            if sub == 0:
                sib_chunk(s - 1, SUBS - 1)
                gather_rider(s)
            else:
                sib_chunk(s, sub - 1)
        return carry

    lax.fori_loop(1, n - 1, ag_step, 0)
    last = n - 1
    for sub in range(SUBS):
        for way in range(2):
            ag_copy(last - 1, sub, way).wait_recv()
        own_chunk(last, sub, False)
        if sub == 0:
            sib_chunk(last - 1, SUBS - 1)
        else:
            sib_chunk(last, sub - 1)
    sib_chunk(last, SUBS - 1)
    for sub in range(SUBS):
        for way in range(2):
            for whose in range(2):
                out_copy(whose, last, sub, way).wait()

    def drain(s, carry):
        for sub in range(SUBS):
            for way in range(2):
                rs_copy(s, sub, way).wait_send()
                ag_copy(s, sub, way).wait_send()
                sib_copy(s, sub, way).wait_send()
        return carry

    lax.fori_loop(0, n - 1, drain, 0)
    for sub in range(SUBS):
        for way in range(2):
            sib_copy(last, sub, way).wait_send()


def ring_scratch(n, seq, d_model, extra):
    width, block = d_model // 4, seq // n
    sub_rows = block // SUBS
    dma = pltpu.SemaphoreType.DMA
    return [
        pltpu.VMEM((2, n, block, width), F32),
        pltpu.VMEM((2, n, block + extra, width), F32),
        pltpu.VMEM((2, 2 * SUBS, sub_rows + extra, width), F32),
        pltpu.VMEM((2, SUBS, 2, sub_rows, width), BF16),
        dma((2, n - 1, SUBS)), dma((2, n - 1, SUBS)), dma((2, n - 1, SUBS)), dma((2, n - 1, SUBS)),
        dma((2, SUBS * n)), dma((2, SUBS * n)), dma((2, SUBS, 2)), pltpu.SemaphoreType.REGULAR,
    ]


def out_kernel(n, o_ref, wo_ref, q_ref, k_ref, v_ref, low_ref, high_ref, x_ref, dout_ref,
               out_ref, dlhs_ref, lhs, rhs, x_rows, dout_rows, do_blk, dk_acc, x32, dkv32, wo32, o_got, wo_got, dq_got, dkv_got,
               row_sem, dout_sem, swap_send, swap_recv, *ring):
    bufs, sems = ring[:4], ring[4:]
    place = ring_kernel_setup(n)
    chip, core, right, left, sib = place
    width = bufs[0].shape[-1]
    half = 2 * width
    block = x_rows.shape[0]
    inner = o_ref.shape[1]
    count = q_ref.shape[0] // ROWS
    x_copy = pltpu.make_async_copy(
        x_ref.at[pl.ds(pl.multiple_of(chip * block, block), block), pl.ds(pl.multiple_of(core * half, 128), half)],
        x_rows, row_sem)

    def dout_copy(i):
        return pltpu.make_async_copy(dout_ref.at[pl.ds(i * ROWS, ROWS), :], dout_rows.at[i % 2], dout_sem.at[i % 2])

    swaps = [remote(src, dst, swap_send.at[k], swap_recv.at[k], sib)
             for k, (src, dst) in enumerate([(wo32, wo_got), (x32, o_got), (x32, dq_got), (dkv32, dkv_got)])]
    x_copy.start()
    dout_copy(0).start()
    wo32[...] = wo_ref[:, pl.ds(pl.multiple_of((1 - core) * half, 128), half)].astype(F32)
    peers_ready()
    swaps[0].start()
    x32[...] = o_ref[...].astype(F32)
    swaps[1].start()
    lhs[:, :inner] = o_ref[...]
    rhs[:inner, :] = wo_ref[:, pl.ds(pl.multiple_of(core * half, 128), half)]
    swaps[0].wait()
    rhs[inner:, :] = wo_got[...].astype(BF16)
    swaps[1].wait()
    lhs[:, inner:] = o_got[...].astype(BF16)

    def partial(rows, way):
        return dot(lhs[rows, :], rhs[:, way * width:(way + 1) * width], (1, 0))

    sub_rows = block // SUBS

    def finish(sub, sums):
        if sub == 0:
            x_copy.wait()
        for way in range(2):
            rows = pl.ds(sub * sub_rows, sub_rows)
            bufs[1][way, 0, rows, :] = sums[way] + x_rows[rows, way * width:(way + 1) * width].astype(F32)

    dv_acc = dkv32.at[:, pl.ds(HEAD_DIM, HEAD_DIM)]

    def ride(step):
        for i in range(step * count // n, (step + 1) * count // n):
            dout_copy(i).wait()
            if i + 1 < count:
                dout_copy(i + 1).start()
            do_blk[...] = dot(dout_rows[i % 2], wo_ref[...], (1, 1)).astype(BF16)
            attn_bwd_rows(i, do_blk, q_ref, k_ref, v_ref, low_ref, high_ref, x32, dk_acc, dv_acc)
        if step == n - 1:
            def turn_back(b, carry):
                rows = pl.ds(pl.multiple_of(b * ROWS, ROWS), ROWS)
                cos_t, sin_t = rope_block(b, low_ref, high_ref)
                dkv32[rows, :HEAD_DIM] = rotate(dk_acc[rows, :], cos_t, -sin_t)
                return carry
            lax.fori_loop(0, count, turn_back, 0)
            swaps[2].start()
            swaps[3].start()

    def rider(step):
        if isinstance(step, int):
            ride(step)
        else:
            for static in range(1, n - 1):
                pl.when(step == static)(lambda static=static: ride(static))

    def gather_rider(step):
        @pl.when(step == n // 2)
        def _():
            swaps[2].wait()
            swaps[3].wait()
            dlhs_ref[:, :inner] = x32[...].astype(BF16)
            dlhs_ref[:, inner:2 * inner] = (dkv32[...] + dkv_got[...]).astype(BF16)
            dlhs_ref[:, 2 * inner:] = dq_got[...].astype(BF16)

    ring_sum(n, place, 0, partial, finish, rider, gather_rider, out_ref, None, bufs, sems)


def grad_kernel(n, lhs, o_ref, wqsib_ref, gain_ref, wq_ref, wk_ref, wv_ref, x_ref, dout_ref, n_ref,
                out_ref, gsum_ref, dw_ref, dwo_ref, n_blk, dout_blk, dw_blk, dwo_blk, blk_sem, dw_sem, rhs, gain, x_rows, dout_rows, unit_buf, stat_buf, gain_acc, row_sem, stat_send, stat_recv, *ring):
    bufs, sems = ring[:4], ring[4:]
    place = ring_kernel_setup(n)
    chip, core, right, left, sib = place
    width = bufs[0].shape[-1]
    block = x_rows.shape[0]
    inner = wq_ref.shape[1]
    half = 2 * width
    row = pl.multiple_of(chip * block, block)
    col = pl.multiple_of(core * half, 128)
    head_cols = pl.ds(pl.multiple_of(chip * HEAD_DIM, HEAD_DIM), HEAD_DIM)
    x_copy = pltpu.make_async_copy(x_ref.at[pl.ds(row, block), :], x_rows, row_sem.at[0])
    dout_copy = pltpu.make_async_copy(dout_ref.at[pl.ds(row, block), pl.ds(col, half)], dout_rows, row_sem.at[1])
    weights = [
        pltpu.make_async_copy(wq_ref.at[pl.ds(col, half), :], rhs.at[:, pl.ds(0, inner)], row_sem.at[2]),
        pltpu.make_async_copy(wk_ref.at[pl.ds(col, half), head_cols], rhs.at[:, pl.ds(inner, HEAD_DIM)], row_sem.at[3]),
        pltpu.make_async_copy(wv_ref.at[pl.ds(col, half), head_cols], rhs.at[:, pl.ds(inner + HEAD_DIM, HEAD_DIM)], row_sem.at[4]),
    ]
    count = n_ref.shape[1] // ROWS

    def loads(j):
        cols = pl.ds(pl.multiple_of(j * ROWS, ROWS), ROWS)
        return [pltpu.make_async_copy(n_ref.at[:, cols], n_blk.at[j % 2], blk_sem.at[0, j % 2]),
                pltpu.make_async_copy(dout_ref.at[:, cols], dout_blk.at[j % 2], blk_sem.at[1, j % 2])]

    def stores(j):
        cols = pl.ds(pl.multiple_of(j * ROWS, ROWS), ROWS)
        return [pltpu.make_async_copy(dw_blk.at[j % 2], dw_ref.at[cols, :], dw_sem.at[0, j % 2]),
                pltpu.make_async_copy(dwo_blk.at[j % 2], dwo_ref.at[:, cols], dw_sem.at[1, j % 2])]

    def weight_block(j):
        for copy in loads(j):
            copy.wait()

        @pl.when(j + 1 < count)
        def _():
            for copy in loads(j + 1):
                copy.start()

        @pl.when(j >= 2)
        def _():
            for copy in stores(j - 2):
                copy.wait()
        dw_blk[j % 2] = dot(n_blk[j % 2], lhs[:, :2 * inner], (0, 0))
        dwo_blk[j % 2] = dot(o_ref[...], dout_blk[j % 2], (0, 0))
        for copy in stores(j):
            copy.start()

    for copy in weights + [x_copy, dout_copy] + loads(0):
        copy.start()
    rhs[:, inner + 2 * HEAD_DIM:] = wqsib_ref[...].astype(BF16)
    gain[...] = gain_ref[:, pl.ds(col, half)].astype(F32)
    for copy in weights:
        copy.wait()
    peers_ready()
    gain_acc[...] = jnp.zeros_like(gain_acc)

    def partial(rows, way):
        return dot(lhs[rows, :], rhs[way * width:(way + 1) * width, :], (1, 1))

    sub_rows = block // SUBS

    def prepare(sub):
        rows = pl.ds(sub * sub_rows, sub_rows)
        x = x_rows[rows, :].astype(F32)
        inv = lax.rsqrt(jnp.mean(x * x, axis=-1, keepdims=True) + NORM_EPS)
        stat_buf[2, rows, :] = jnp.broadcast_to(inv, (sub_rows, HEAD_DIM))
        mine = x_rows[rows, pl.ds(col, half)].astype(F32)
        unit_buf[rows, :] = mine * inv

    def rider(step):
        if isinstance(step, int) and step == 0:
            x_copy.wait()
            dout_copy.wait()
            for sub in range(SUBS):
                prepare(sub)
        elif not isinstance(step, int):
            pl.when(step - 1 < count)(lambda: weight_block(step - 1))

    def gather_rider(step):
        pl.when(step + n - 3 < count)(lambda: weight_block(step + n - 3))

    def stat_copy(sub):
        rows = pl.ds(sub * sub_rows, sub_rows)
        return remote(stat_buf.at[0, rows, :], stat_buf.at[1, rows, :], stat_send.at[sub], stat_recv.at[sub], sib)

    def finish(sub, sums):
        rows = pl.ds(sub * sub_rows, sub_rows)
        ag_buf = bufs[1]
        total = jnp.zeros((sub_rows, 1), F32)
        for way in range(2):
            cols = slice(way * width, (way + 1) * width)
            unit = unit_buf[rows, cols]
            prod = sums[way] * unit
            total = total + jnp.sum(prod * gain[:, cols], axis=-1, keepdims=True)
            gsum = jnp.sum(prod.reshape(sub_rows // 8, 8, width), axis=0)
            ag_buf[way, 0, pl.ds(block, 8), :] = gsum if sub == 0 else gsum + ag_buf[way, 0, pl.ds(block, 8), :]
            ag_buf[way, 0, rows, :] = sums[way]
        stat_buf[0, rows, :] = jnp.broadcast_to(total, (sub_rows, HEAD_DIM))
        stat_copy(sub).start()
        stat_copy(sub).wait()
        mean = (stat_buf[0, rows, 0:1] + stat_buf[1, rows, 0:1]) * (1.0 / (2 * half))
        inv = stat_buf[2, rows, 0:1]
        for way in range(2):
            cols = slice(way * width, (way + 1) * width)
            scaled = ag_buf[way, 0, rows, :] * gain[:, cols]
            ag_buf[way, 0, rows, :] = dout_rows[rows, cols].astype(F32) + inv * (scaled - unit_buf[rows, cols] * mean)

    ring_sum(n, place, 8, partial, finish, rider, gather_rider, out_ref, gain_acc, bufs, sems)
    for j in (count - 2, count - 1):
        for copy in stores(j):
            copy.wait()
    for way in range(2):
        gsum_ref[core, way] = jnp.sum(gain_acc[0, way], axis=0, keepdims=True)
        gsum_ref[1 - core, way] = jnp.sum(gain_acc[1, way], axis=0, keepdims=True)


def final_kernel(*refs):
    half = len(refs) // 2
    for src, dst in zip(refs[:half], refs[half:]):
        dst[...] = src[...]


def final(out, gh, dw, dwo):
    seq, d = out.shape
    inner = dwo.shape[0]
    steps = seq // ROWS
    row = lambda a: pl.BlockSpec((a.shape[0] // steps, a.shape[1]), lambda j: (j, 0))
    part = lambda w, at: pl.BlockSpec((d // steps, w), lambda j: (j, at))
    shape = jax.ShapeDtypeStruct
    return pl.pallas_call(
        final_kernel, grid=(steps,),
        in_specs=[row(out), row(gh), part(inner, 0), part(HEAD_DIM, inner // HEAD_DIM), part(HEAD_DIM, inner // HEAD_DIM + 1), row(dwo)],
        out_specs=[row(out), row(gh), part(inner, 0), part(HEAD_DIM, 0), part(HEAD_DIM, 0), row(dwo)],
        out_shape=[shape(out.shape, BF16), shape(gh.shape, BF16), shape((d, inner), F32), shape((d, HEAD_DIM), F32),
                   shape((d, HEAD_DIM), F32), shape(dwo.shape, F32)],
        compiler_params=pltpu.CompilerParams(vmem_limit_bytes=VMEM_LIMIT),
        cost_estimate=pl.CostEstimate(flops=seq * d, bytes_accessed=12 * seq * d, transcendentals=0),
        name='final')(out, gh, dw, dw, dw, dwo)


def out_sum(n, o, wo, q, k, v, low, high, x, dout):
    seq, d_model = x.shape
    half, block, inner = d_model // 2, seq // n, o.shape[1]
    vmem, hbm = pl.BlockSpec(memory_space=pltpu.VMEM), pl.BlockSpec(memory_space=pl.ANY)
    shape = jax.ShapeDtypeStruct
    dma = pltpu.SemaphoreType.DMA
    rows32 = pltpu.VMEM((seq, inner), F32)
    wide32 = pltpu.VMEM((inner, half), F32)
    return pl.pallas_call(
        functools.partial(out_kernel, n),
        out_shape=[shape((seq, d_model), BF16), shape((seq, 2 * inner + 2 * HEAD_DIM), BF16)],
        in_specs=[vmem] * 7 + [hbm] * 2, out_specs=[hbm, vmem],
        scratch_shapes=[pltpu.VMEM((seq, 2 * inner), BF16), pltpu.VMEM((2 * inner, half), BF16),
                        pltpu.VMEM((block, half), BF16), pltpu.VMEM((2, ROWS, d_model), BF16), pltpu.VMEM((ROWS, inner), BF16),
                        pltpu.VMEM((seq, HEAD_DIM), F32), rows32, rows32, wide32, rows32, wide32, rows32, rows32,
                        dma, dma((2,)), dma((4,)), dma((4,))]
        + ring_scratch(n, seq, d_model, 0),
        compiler_params=pltpu.CompilerParams(collective_id=1, has_side_effects=True, vmem_limit_bytes=VMEM_LIMIT),
        cost_estimate=pl.CostEstimate(flops=10 * seq * seq * HEAD_DIM, bytes_accessed=4 * seq * d_model, transcendentals=seq * seq),
        name='out_sum')(o, wo, q, k, v, low, high, x, dout)


def grad_sum(n, dlhs, o, wq_sib, gain, wq, wk, wv, x, dout, normed):
    seq, d_model = x.shape
    half, block, width = d_model // 2, seq // n, d_model // 4
    kdim, inner = dlhs.shape[1], o.shape[1]
    vmem, hbm = pl.BlockSpec(memory_space=pltpu.VMEM), pl.BlockSpec(memory_space=pl.ANY)
    shape = jax.ShapeDtypeStruct
    dma = pltpu.SemaphoreType.DMA
    return pl.pallas_call(
        functools.partial(grad_kernel, n),
        out_shape=[shape((seq, d_model), BF16), shape((2, 2, 1, width), F32), shape((d_model, 2 * inner), F32), shape((inner, d_model), F32)],
        in_specs=[vmem] * 4 + [hbm] * 6, out_specs=[hbm, vmem, hbm, hbm],
        scratch_shapes=[pltpu.VMEM((2, seq, ROWS), BF16), pltpu.VMEM((2, seq, ROWS), BF16),
                        pltpu.VMEM((2, ROWS, 2 * inner), F32), pltpu.VMEM((2, inner, ROWS), F32), dma((2, 2)), dma((2, 2)),
                        pltpu.VMEM((half, kdim), BF16), pltpu.VMEM((1, half), F32),
                        pltpu.VMEM((block, d_model), BF16), pltpu.VMEM((block, half), BF16), pltpu.VMEM((block, half), F32),
                        pltpu.VMEM((3, block, HEAD_DIM), F32), pltpu.VMEM((2, 2, 8, width), F32),
                        dma((5,)), dma((SUBS,)), dma((SUBS,))]
        + ring_scratch(n, seq, d_model, 8),
        compiler_params=pltpu.CompilerParams(collective_id=2, has_side_effects=True, vmem_limit_bytes=VMEM_LIMIT),
        cost_estimate=pl.CostEstimate(flops=4 * seq * kdim * half, bytes_accessed=4 * seq * d_model, transcendentals=0),
        name='grad_sum')(dlhs, o, wq_sib, gain, wq, wk, wv, x, dout, normed)


def solution(mesh):
    tp_size = mesh.shape['tp']
    chips = tp_size // 2
    swap = [(source, source ^ 1) for source in range(tp_size)]

    def block_fn(hidden, grad_out, norm_gain, w_query, w_key, w_value, w_out):
        batch, seq_len, d_model = hidden.shape
        half = d_model // 2
        tp_index = lax.axis_index('tp')
        kv_index, core = tp_index // 2, tp_index % 2
        low, high = rope_tables(seq_len // ROWS)
        x, dout = hidden[0], grad_out[0]
        gain = norm_gain[None, :]
        scalars = jnp.stack([kv_index, 1 - core])
        n, q, k, v, o, wq32 = front(scalars, x, gain, w_query, w_key, w_value, low, high)
        wq_sib = lax.ppermute(wq32, 'tp', swap)
        out, dlhs = out_sum(chips, o, w_out, q, k, v, low, high, x, dout)
        gh, gain_sum, dw, dwo = grad_sum(chips, dlhs, o, wq_sib, gain, w_query, w_key, w_value, x, dout, n)
        out, gh, grad_w_query, grad_w_key, grad_w_value, grad_w_out = final(out, gh, dw, dwo)
        return out[None], gh[None], gain_sum.reshape(-1), grad_w_query, grad_w_key, grad_w_value, grad_w_out

    act_spec = P('dp', None, None)
    return jax.shard_map(
        block_fn, mesh=mesh,
        in_specs=(act_spec, act_spec, P(None), P(None, 'tp'), P(None, None), P(None, None), P('tp', None)),
        out_specs=(act_spec, act_spec, P('dp'), P('dp', 'tp'), P('dp', 'tp'), P('dp', 'tp'), P(('dp', 'tp'), None)),
        check_vma=False)
```

```python
import functools
import math
import jax
import jax.numpy as jnp
import numpy as np
from jax import lax
from jax.experimental import pallas as pl
from jax.experimental.pallas import tpu as pltpu
from jax.sharding import PartitionSpec as P

HEAD_DIM = 128
NORM_EPS = 1.0e-5
ROPE_BASE = 10000.0
MASK_VALUE = -1.0e30
SCORE_SCALE = 1.0 / math.sqrt(HEAD_DIM)
EXP2_SCALE = SCORE_SCALE * math.log2(math.e)
ROWS = 256
WIDE = 512
BF16 = jnp.bfloat16
F32 = jnp.float32
VMEM_LIMIT = 66 * 10**6


def dot(a, b, contract):
    return lax.dot_general(a, b, ((contract[:1], contract[1:]), ((), ())), preferred_element_type=F32)


def rope_tables(count):
    def table(positions):
        inv_freq = ROPE_BASE ** (-np.arange(0, HEAD_DIM, 2, dtype=np.float64) / HEAD_DIM)
        angles = positions[:, None] * inv_freq[None, :]
        cos_t = np.repeat(np.cos(angles), 2, axis=1)
        sin_t = np.stack([-np.sin(angles), np.sin(angles)], axis=-1).reshape(cos_t.shape)
        return np.stack([cos_t, sin_t]).astype(np.float32)
    return table(np.arange(ROWS, dtype=np.float64)), table(ROWS * np.arange(count, dtype=np.float64))


def rope_block(b, low_ref, high_ref):
    cos_b, sin_b = high_ref[0, pl.ds(b, 1), :], high_ref[1, pl.ds(b, 1), :]
    cos_l, sin_l = low_ref[0], low_ref[1]
    return cos_b * cos_l - sin_b * sin_l, sin_b * cos_l + cos_b * sin_l


def rotate(t, cos_t, sin_t):
    even = lax.broadcasted_iota(jnp.int32, t.shape, 1) % 2 == 0
    swapped = jnp.where(even, pltpu.roll(t, HEAD_DIM - 1, 1), pltpu.roll(t, 1, 1))
    return t * cos_t + swapped * sin_t


def front_kernel(kv_ref, x_ref, gain_ref, wq_ref, wk_ref, wv_ref, low_ref, high_ref,
                 n_ref, q_ref, k_ref, v_ref, wq32_ref, wqkv):
    i = pl.program_id(0)
    half = wq32_ref.shape[0]

    @pl.when(i == 0)
    def _():
        wqkv[:, :2 * HEAD_DIM] = wq_ref[...]
        wqkv[:, 2 * HEAD_DIM:3 * HEAD_DIM] = wk_ref[...]
        wqkv[:, 3 * HEAD_DIM:] = wv_ref[...]
        wq32_ref[...] = wq_ref[pl.ds(pl.multiple_of(kv_ref[1] * half, half), half), :].astype(F32)

    parts = []
    for r in range(0, WIDE, ROWS):
        rows = slice(r, r + ROWS)
        x = x_ref[rows, :].astype(F32)
        inv = lax.rsqrt(jnp.mean(x * x, axis=-1, keepdims=True) + NORM_EPS)
        n_ref[rows, :] = (x * inv * gain_ref[...].astype(F32)).astype(BF16)
        parts.append(rope_block(i * (WIDE // ROWS) + r // ROWS, low_ref, high_ref))
    qkv = dot(n_ref[...], wqkv[...], (1, 0))
    cos_t, sin_t = (jnp.concatenate([p[t] for p in parts], axis=0) for t in range(2))
    q0 = rotate(qkv[:, :HEAD_DIM], cos_t, sin_t).astype(BF16)
    q1 = rotate(qkv[:, HEAD_DIM:2 * HEAD_DIM], cos_t, sin_t).astype(BF16)
    k = rotate(qkv[:, 2 * HEAD_DIM:3 * HEAD_DIM], cos_t, sin_t).astype(BF16)
    v = qkv[:, 3 * HEAD_DIM:].astype(BF16)
    q_ref[:, :HEAD_DIM] = q0
    q_ref[:, HEAD_DIM:] = q1
    k_ref[...] = k
    v_ref[...] = v


def front(scalars, x, gain, wq, wk, wv, low, high):
    seq, d = x.shape
    row = lambda w: pl.BlockSpec((WIDE, w), lambda i, kv: (i, 0))
    whole = lambda shape: pl.BlockSpec(shape, lambda i, kv: (0,) * len(shape))
    head = pl.BlockSpec((d, HEAD_DIM), lambda i, kv: (0, kv[0]))
    widths = (d, 2 * HEAD_DIM, HEAD_DIM, HEAD_DIM)
    return pl.pallas_call(
        front_kernel,
        grid_spec=pltpu.PrefetchScalarGridSpec(
            num_scalar_prefetch=1, grid=(seq // WIDE,),
            in_specs=[row(d), whole(gain.shape), whole(wq.shape), head, head, whole(low.shape), whole(high.shape)],
            out_specs=[row(w) for w in widths] + [whole((d // 2, wq.shape[1]))],
            scratch_shapes=[pltpu.VMEM((d, 4 * HEAD_DIM), BF16)]),
        out_shape=[jax.ShapeDtypeStruct((seq, w), BF16) for w in widths] + [jax.ShapeDtypeStruct((d // 2, wq.shape[1]), F32)],
        compiler_params=pltpu.CompilerParams(vmem_limit_bytes=VMEM_LIMIT),
        cost_estimate=pl.CostEstimate(flops=2 * seq * d * 4 * HEAD_DIM, bytes_accessed=5 * seq * d, transcendentals=0),
        name='front')(scalars, x, gain, wq, wk, wv, low, high)


def attn_fwd_rows(c, q_ref, k_ref, v_ref, o_ref):
    lo, hi = c * WIDE, (c + 1) * WIDE

    def block(r, carry):
        rows = pl.ds(pl.multiple_of(lo + r * ROWS, ROWS), ROWS)
        q2 = jnp.concatenate([q_ref[rows, :HEAD_DIM], q_ref[rows, HEAD_DIM:]], axis=0)
        row_id = lax.broadcasted_iota(jnp.int32, (2 * ROWS, WIDE), 0) % ROWS + r * ROWS
        causal = row_id >= lax.broadcasted_iota(jnp.int32, (2 * ROWS, WIDE), 1)
        s_diag = jnp.where(causal, dot(q2, k_ref[lo:hi, :], (1, 1)), MASK_VALUE)
        m = jnp.max(s_diag, axis=-1, keepdims=True)
        if lo:
            s_pre = dot(q2, k_ref[:lo, :], (1, 1))
            m = jnp.maximum(m, jnp.max(s_pre, axis=-1, keepdims=True))
        p_diag = jnp.exp2((s_diag - m) * EXP2_SCALE)
        total = jnp.sum(p_diag, axis=-1, keepdims=True)
        if lo:
            p_pre = jnp.exp2((s_pre - m) * EXP2_SCALE)
            total = total + jnp.sum(p_pre, axis=-1, keepdims=True)
        scale = 1.0 / total
        o2 = dot((p_diag * scale).astype(BF16), v_ref[lo:hi, :], (1, 0))
        if lo:
            o2 = o2 + dot((p_pre * scale).astype(BF16), v_ref[:lo, :], (1, 0))
        o_ref[rows, :HEAD_DIM] = o2[:ROWS].astype(BF16)
        o_ref[rows, HEAD_DIM:] = o2[ROWS:].astype(BF16)
        return carry

    lax.fori_loop(0, WIDE // ROWS, block, 0)


def attn_bwd_rows(i, c, do_both, q_ref, k_ref, v_ref, low_ref, high_ref, dq32, dk_acc, dv_acc):
    lo, hi = c * WIDE, (c + 1) * WIDE
    rows = pl.ds(pl.multiple_of(i * ROWS, ROWS), ROWS)
    query_id = lax.broadcasted_iota(jnp.int32, (WIDE, ROWS), 1) + (i * ROWS - lo)
    causal = lax.broadcasted_iota(jnp.int32, (WIDE, ROWS), 0) <= query_id

    def one_head(head, carry):
        cols = pl.ds(pl.multiple_of(head * HEAD_DIM, HEAD_DIM), HEAD_DIM)
        q, do = q_ref[rows, cols], do_both[:, cols]
        k_all, v_all = k_ref[:hi, :], v_ref[:hi, :]
        s_t = dot(k_all, q, (1, 1))
        s_diag = jnp.where(causal, s_t[lo:], MASK_VALUE)
        s_t = jnp.concatenate([s_t[:lo], s_diag], axis=0) if lo else s_diag
        m = jnp.max(s_t, axis=0, keepdims=True)
        p = jnp.exp2((s_t - m) * EXP2_SCALE)
        p = p * (1.0 / jnp.sum(p, axis=0, keepdims=True))
        dp = dot(v_all, do, (1, 1))
        delta = jnp.sum(p * dp, axis=0, keepdims=True)
        ds = (p * (dp - delta) * SCORE_SCALE).astype(BF16)
        dv_acc[:hi, :] += dot(p.astype(BF16), do, (1, 0))
        dk_acc[:hi, :] += dot(ds, q, (1, 0))
        dq = dot(ds, k_all, (0, 0))
        cos_t, sin_t = rope_block(i, low_ref, high_ref)
        dq32[rows, cols] = rotate(dq, cos_t, -sin_t).astype(BF16).astype(F32)
        return carry

    lax.fori_loop(0, 2, one_head, 0)


SUBS = 4


def ring_kernel_setup(n):
    me = lax.axis_index('tp')
    chip, core = me // 2, me % 2
    right = (chip + 1) % n * 2 + core
    left = (chip + n - 1) % n * 2 + core
    sib = me + 1 - 2 * core
    barrier = pltpu.get_barrier_semaphore()
    for peer in (right, left, sib):
        pl.semaphore_signal(barrier, inc=1, device_id={'tp': peer}, device_id_type=pl.DeviceIdType.MESH)
    return chip, core, right, left, sib


def peers_ready():
    pl.semaphore_wait(pltpu.get_barrier_semaphore(), 3)


def remote(src, dst, send, recv, peer):
    return pltpu.make_async_remote_copy(src_ref=src, dst_ref=dst, send_sem=send, recv_sem=recv,
                                        device_id={'tp': peer}, device_id_type=pl.DeviceIdType.MESH)


def owned_rows(n, sub_rows, chip, sub):
    return pl.ds(pl.multiple_of((sub * n + chip) * sub_rows, sub_rows), sub_rows)


def ring_sum(n, place, extra, partial, ready, finish, rider, gather_rider, out_ref, gain_acc, bufs, sems):
    chip, core, right, left, sib = place
    rs_buf, ag_buf, sib_buf, obuf = bufs
    rs_send, rs_recv, ag_send, ag_recv, sib_send, sib_recv, out_sem, credit = sems
    width = rs_buf.shape[-1]
    block = out_ref.shape[0] // n
    sub_rows = block // SUBS
    half = 2 * width
    peers = (right, left)

    def part(slot_ref, sub, with_extra):
        return slot_ref.at[pl.ds(sub * sub_rows, sub_rows + (extra if with_extra and sub == SUBS - 1 else 0)), :]

    def rs_copy(s, sub, way):
        return remote(part(rs_buf.at[way, s], sub, False), part(rs_buf.at[way, s + 1], sub, False),
                      rs_send.at[way, s, sub], rs_recv.at[way, s, sub], peers[way])

    def ag_copy(s, sub, way):
        return remote(part(ag_buf.at[way, s], sub, True), part(ag_buf.at[way, s + 1], sub, True),
                      ag_send.at[way, s, sub], ag_recv.at[way, s, sub], peers[way])

    def sib_copy(s, sub, way):
        rows = sub_rows + (extra if sub == SUBS - 1 else 0)
        k = SUBS * s + sub
        return remote(part(ag_buf.at[way, s], sub, True), sib_buf.at[way, k % (2 * SUBS), pl.ds(0, rows), :],
                      sib_send.at[way, k], sib_recv.at[way, k], sib)

    def my_part(dest, sub, way):
        return partial(owned_rows(n, sub_rows, dest, sub), way)

    def dest_of(s, way):
        return (chip + n - 1 - s) % n if way == 0 else (chip + 1 + s) % n

    def local(ref, sub):
        return pl.ds(sub * sub_rows, sub_rows)

    for sub in range(SUBS):
        ready(sub)
        for way in range(2):
            rs_buf[way, 0, local(rs_buf, sub), :] = my_part(dest_of(0, way), sub, way)
            rs_copy(0, sub, way).start()

    def rs_step(s, carry):
        for sub in range(SUBS):
            for way in range(2):
                term = my_part(dest_of(s, way), sub, way)
                rs_copy(s - 1, sub, way).wait_recv()
                rs_buf[way, s, local(rs_buf, sub), :] += term
                rs_copy(s, sub, way).start()
            if sub == 0:
                rider(s)
        return carry

    lax.fori_loop(1, n - 1, rs_step, 0)

    def out_copy(whose, s, sub, way):
        b = (chip + n - s) % n if way == 0 else (chip + s) % n
        col = (core if whose == 0 else 1 - core) * half + way * width
        dst = out_ref.at[owned_rows(n, sub_rows, b, sub), pl.ds(pl.multiple_of(col, 128), width)]
        return pltpu.make_async_copy(obuf.at[whose, sub, way], dst, out_sem.at[whose, sub, way])

    def emit(whose, s, sub, way, values):
        @pl.when(s >= 1)
        def _():
            out_copy(whose, s - 1, sub, way).wait()
        obuf[whose, sub, way] = values.astype(BF16)
        out_copy(whose, s, sub, way).start()

    def own_chunk(s, sub, forward):
        @pl.when(s >= 2)
        def _():
            pl.semaphore_wait(credit, 1)
        for way in range(2):
            if forward:
                ag_copy(s, sub, way).start()
            sib_copy(s, sub, way).start()
        for way in range(2):
            emit(0, s, sub, way, ag_buf[way, s, local(ag_buf, sub), :])
            if extra and sub == SUBS - 1:
                gain_acc[0, way] += ag_buf[way, s, pl.ds(block, extra), :]

    def sib_chunk(s, sub):
        k = SUBS * s + sub
        for way in range(2):
            sib_copy(s, sub, way).wait_recv()
            emit(1, s, sub, way, sib_buf[way, k % (2 * SUBS), pl.ds(0, sub_rows), :])
            if extra and sub == SUBS - 1:
                gain_acc[1, way] += sib_buf[way, k % (2 * SUBS), pl.ds(sub_rows, extra), :]

        @pl.when(s < n - 2)
        def _():
            pl.semaphore_signal(credit, inc=1, device_id={'tp': sib}, device_id_type=pl.DeviceIdType.MESH)

    for sub in range(SUBS):
        terms = [my_part(chip, sub, way) for way in range(2)]
        for way in range(2):
            rs_copy(n - 2, sub, way).wait_recv()
        finish(sub, [rs_buf[way, n - 1, local(rs_buf, sub), :] + terms[way] for way in range(2)])
        own_chunk(0, sub, True)
        if sub:
            sib_chunk(0, sub - 1)

    def ag_step(s, carry):
        for sub in range(SUBS):
            for way in range(2):
                ag_copy(s - 1, sub, way).wait_recv()
            own_chunk(s, sub, True)
            if sub == 0:
                sib_chunk(s - 1, SUBS - 1)
                gather_rider(s)
            else:
                sib_chunk(s, sub - 1)
        return carry

    lax.fori_loop(1, n - 1, ag_step, 0)
    last = n - 1
    for sub in range(SUBS):
        for way in range(2):
            ag_copy(last - 1, sub, way).wait_recv()
        own_chunk(last, sub, False)
        if sub == 0:
            sib_chunk(last - 1, SUBS - 1)
        else:
            sib_chunk(last, sub - 1)
    sib_chunk(last, SUBS - 1)
    for sub in range(SUBS):
        for way in range(2):
            for whose in range(2):
                out_copy(whose, last, sub, way).wait()

    def drain(s, carry):
        for sub in range(SUBS):
            for way in range(2):
                rs_copy(s, sub, way).wait_send()
                ag_copy(s, sub, way).wait_send()
                sib_copy(s, sub, way).wait_send()
        return carry

    lax.fori_loop(0, n - 1, drain, 0)
    for sub in range(SUBS):
        for way in range(2):
            sib_copy(last, sub, way).wait_send()


def ring_scratch(n, seq, d_model, extra):
    width, block = d_model // 4, seq // n
    sub_rows = block // SUBS
    dma = pltpu.SemaphoreType.DMA
    return [
        pltpu.VMEM((2, n, block, width), F32),
        pltpu.VMEM((2, n, block + extra, width), F32),
        pltpu.VMEM((2, 2 * SUBS, sub_rows + extra, width), F32),
        pltpu.VMEM((2, SUBS, 2, sub_rows, width), BF16),
        dma((2, n - 1, SUBS)), dma((2, n - 1, SUBS)), dma((2, n - 1, SUBS)), dma((2, n - 1, SUBS)),
        dma((2, SUBS * n)), dma((2, SUBS * n)), dma((2, SUBS, 2)), pltpu.SemaphoreType.REGULAR,
    ]


def out_kernel(n, wo_ref, q_ref, k_ref, v_ref, low_ref, high_ref, x_ref, dout_ref,
               out_ref, o_ref, dlhs_ref, lhs, rhs, x_rows, dout_rows, do_blk, dk_acc, x32, dkv32, wo32, o_got, wo_got, dq_got, dkv_got,
               row_sem, dout_sem, swap_send, swap_recv, o_send, o_recv, *ring):
    bufs, sems = ring[:4], ring[4:]
    place = ring_kernel_setup(n)
    chip, core, right, left, sib = place
    width = bufs[0].shape[-1]
    half = 2 * width
    block = x_rows.shape[0]
    sub_rows = block // SUBS
    inner = o_ref.shape[1]
    wide = n * sub_rows
    my_cols = pl.ds(pl.multiple_of(core * half, 128), half)

    def x_copy(sub):
        return pltpu.make_async_copy(x_ref.at[owned_rows(n, sub_rows, chip, sub), my_cols],
                                     x_rows.at[pl.ds(sub * sub_rows, sub_rows), :], row_sem.at[sub])

    def dout_copy(i):
        return pltpu.make_async_copy(dout_ref.at[pl.ds(pl.multiple_of(i * ROWS, ROWS), ROWS), :], dout_rows.at[i % 2], dout_sem.at[i % 2])

    swaps = [remote(src, dst, swap_send.at[k], swap_recv.at[k], sib)
             for k, (src, dst) in enumerate([(wo32, wo_got), (x32, dq_got), (dkv32, dkv_got)])]

    def o_swap(w):
        rows = pl.ds(w * wide, wide)
        return remote(x32.at[rows, :], o_got.at[rows, :], o_send.at[w], o_recv.at[w], sib)

    def forward(w):
        rows = pl.ds(w * wide, wide)
        attn_fwd_rows(w, q_ref, k_ref, v_ref, o_ref)
        x32[rows, :] = o_ref[rows, :].astype(F32)
        o_swap(w).start()
        lhs[rows, :inner] = o_ref[rows, :]

    for sub in range(SUBS):
        x_copy(sub).start()
    dout_copy(0).start()
    wo32[...] = wo_ref[:, pl.ds(pl.multiple_of((1 - core) * half, 128), half)].astype(F32)
    peers_ready()
    swaps[0].start()
    forward(0)
    rhs[:inner, :] = wo_ref[:, my_cols]
    swaps[0].wait()
    rhs[inner:, :] = wo_got[...].astype(BF16)

    def ready(sub):
        if sub + 1 < SUBS:
            forward(sub + 1)
        o_swap(sub).wait()
        rows = pl.ds(sub * wide, wide)
        lhs[rows, inner:] = o_got[rows, :].astype(BF16)
        if sub == SUBS - 1:
            dk_acc[...] = jnp.zeros_like(dk_acc)
            dkv32[:, HEAD_DIM:] = jnp.zeros_like(dk_acc)

    def partial(rows, way):
        return dot(lhs[rows, :], rhs[:, way * width:(way + 1) * width], (1, 0))

    def finish(sub, sums):
        x_copy(sub).wait()
        for way in range(2):
            rows = pl.ds(sub * sub_rows, sub_rows)
            bufs[1][way, 0, rows, :] = sums[way] + x_rows[rows, way * width:(way + 1) * width].astype(F32)

    dv_acc = dkv32.at[:, pl.ds(HEAD_DIM, HEAD_DIM)]
    count = q_ref.shape[0] // ROWS
    per_wide = WIDE // ROWS

    def ride(i, wides):
        dout_copy(i).wait()

        @pl.when(i + 1 < count)
        def _():
            dout_copy(i + 1).start()
        do_blk[...] = dot(dout_rows[i % 2], wo_ref[...], (1, 1)).astype(BF16)
        for c in wides:
            pl.when(i // per_wide == c)(
                lambda c=c: attn_bwd_rows(i, c, do_blk, q_ref, k_ref, v_ref, low_ref, high_ref, x32, dk_acc, dv_acc))

    early = n - 2

    def rider(step):
        ride(step - 1, range((early - 1) // per_wide + 1))

    def gather_rider(step):
        @pl.when(step <= count - early)
        def _():
            ride(early - 1 + step, range(early // per_wide, count // per_wide))

        @pl.when(step == count - early + 1)
        def _():
            def turn_back(b, carry):
                rows = pl.ds(pl.multiple_of(b * ROWS, ROWS), ROWS)
                cos_t, sin_t = rope_block(b, low_ref, high_ref)
                dkv32[rows, :HEAD_DIM] = rotate(dk_acc[rows, :], cos_t, -sin_t)
                return carry
            lax.fori_loop(0, count, turn_back, 0)
            swaps[1].start()
            swaps[2].start()

        @pl.when(step == n - 2)
        def _():
            swaps[1].wait()
            swaps[2].wait()
            dlhs_ref[:, :inner] = x32[...].astype(BF16)
            dlhs_ref[:, inner:2 * inner] = (dkv32[...] + dkv_got[...]).astype(BF16)
            dlhs_ref[:, 2 * inner:] = dq_got[...].astype(BF16)

    ring_sum(n, place, 0, partial, ready, finish, rider, gather_rider, out_ref, None, bufs, sems)


def grad_kernel(n, lhs, o_ref, wqsib_ref, gain_ref, wq_ref, wk_ref, wv_ref, x_ref, dout_ref, n_ref,
                out_ref, gsum_ref, dw_ref, dwo_ref, n_blk, dout_blk, dw_blk, dwo_blk, blk_sem, dw_sem, rhs, gain, x_rows, dout_rows, unit_buf, stat_buf, gain_acc, row_sem, stat_send, stat_recv, *ring):
    bufs, sems = ring[:4], ring[4:]
    place = ring_kernel_setup(n)
    chip, core, right, left, sib = place
    width = bufs[0].shape[-1]
    block = x_rows.shape[0]
    inner = wq_ref.shape[1]
    half = 2 * width
    col = pl.multiple_of(core * half, 128)
    head_cols = pl.ds(pl.multiple_of(chip * HEAD_DIM, HEAD_DIM), HEAD_DIM)
    sub_rows = block // SUBS
    rows_copies = []
    for sub in range(SUBS):
        src, dst = owned_rows(n, sub_rows, chip, sub), pl.ds(sub * sub_rows, sub_rows)
        rows_copies += [pltpu.make_async_copy(x_ref.at[src, :], x_rows.at[dst, :], row_sem.at[3 + 2 * sub]),
                        pltpu.make_async_copy(dout_ref.at[src, pl.ds(col, half)], dout_rows.at[dst, :], row_sem.at[4 + 2 * sub])]
    weights = [
        pltpu.make_async_copy(wq_ref.at[pl.ds(col, half), :], rhs.at[:, pl.ds(0, inner)], row_sem.at[0]),
        pltpu.make_async_copy(wk_ref.at[pl.ds(col, half), head_cols], rhs.at[:, pl.ds(inner, HEAD_DIM)], row_sem.at[1]),
        pltpu.make_async_copy(wv_ref.at[pl.ds(col, half), head_cols], rhs.at[:, pl.ds(inner + HEAD_DIM, HEAD_DIM)], row_sem.at[2]),
    ]
    count = n_ref.shape[1] // ROWS

    def loads(j):
        cols = pl.ds(pl.multiple_of(j * ROWS, ROWS), ROWS)
        return [pltpu.make_async_copy(n_ref.at[:, cols], n_blk.at[j % 2], blk_sem.at[0, j % 2]),
                pltpu.make_async_copy(dout_ref.at[:, cols], dout_blk.at[j % 2], blk_sem.at[1, j % 2])]

    def stores(j):
        cols = pl.ds(pl.multiple_of(j * ROWS, ROWS), ROWS)
        return [pltpu.make_async_copy(dw_blk.at[j % 2], dw_ref.at[cols, :], dw_sem.at[0, j % 2]),
                pltpu.make_async_copy(dwo_blk.at[j % 2], dwo_ref.at[:, cols], dw_sem.at[1, j % 2])]

    def weight_block(j):
        for copy in loads(j):
            copy.wait()

        @pl.when(j + 1 < count)
        def _():
            for copy in loads(j + 1):
                copy.start()

        @pl.when(j >= 2)
        def _():
            for copy in stores(j - 2):
                copy.wait()
        dw_blk[j % 2] = dot(n_blk[j % 2], lhs[:, :2 * inner], (0, 0))
        dwo_blk[j % 2] = dot(o_ref[...], dout_blk[j % 2], (0, 0))
        for copy in stores(j):
            copy.start()

    for copy in weights + rows_copies + loads(0):
        copy.start()
    rhs[:, inner + 2 * HEAD_DIM:] = wqsib_ref[...].astype(BF16)
    gain[...] = gain_ref[:, pl.ds(col, half)].astype(F32)
    for copy in weights:
        copy.wait()
    peers_ready()
    gain_acc[...] = jnp.zeros_like(gain_acc)

    def partial(rows, way):
        return dot(lhs[rows, :], rhs[way * width:(way + 1) * width, :], (1, 1))

    def prepare(sub):
        rows = pl.ds(sub * sub_rows, sub_rows)
        x = x_rows[rows, :].astype(F32)
        inv = lax.rsqrt(jnp.mean(x * x, axis=-1, keepdims=True) + NORM_EPS)
        stat_buf[2, rows, :] = jnp.broadcast_to(inv, (sub_rows, HEAD_DIM))
        mine = x_rows[rows, pl.ds(col, half)].astype(F32)
        unit_buf[rows, :] = mine * inv

    def ready(sub):
        if sub == SUBS - 1:
            for copy in rows_copies:
                copy.wait()

    def rider(step):
        @pl.when(step == 1)
        def _():
            for sub in range(SUBS):
                prepare(sub)
        pl.when(step - 1 < count)(lambda: weight_block(step - 1))

    def gather_rider(step):
        pl.when(step + n - 3 < count)(lambda: weight_block(step + n - 3))

    def stat_copy(sub):
        rows = pl.ds(sub * sub_rows, sub_rows)
        return remote(stat_buf.at[0, rows, :], stat_buf.at[1, rows, :], stat_send.at[sub], stat_recv.at[sub], sib)

    def finish(sub, sums):
        rows = pl.ds(sub * sub_rows, sub_rows)
        ag_buf = bufs[1]
        total = jnp.zeros((sub_rows, 1), F32)
        for way in range(2):
            cols = slice(way * width, (way + 1) * width)
            unit = unit_buf[rows, cols]
            prod = sums[way] * unit
            total = total + jnp.sum(prod * gain[:, cols], axis=-1, keepdims=True)
            gsum = jnp.sum(prod.reshape(sub_rows // 8, 8, width), axis=0)
            ag_buf[way, 0, pl.ds(block, 8), :] = gsum if sub == 0 else gsum + ag_buf[way, 0, pl.ds(block, 8), :]
            ag_buf[way, 0, rows, :] = sums[way]
        stat_buf[0, rows, :] = jnp.broadcast_to(total, (sub_rows, HEAD_DIM))
        stat_copy(sub).start()
        stat_copy(sub).wait()
        mean = (stat_buf[0, rows, 0:1] + stat_buf[1, rows, 0:1]) * (1.0 / (2 * half))
        inv = stat_buf[2, rows, 0:1]
        for way in range(2):
            cols = slice(way * width, (way + 1) * width)
            scaled = ag_buf[way, 0, rows, :] * gain[:, cols]
            ag_buf[way, 0, rows, :] = dout_rows[rows, cols].astype(F32) + inv * (scaled - unit_buf[rows, cols] * mean)

    ring_sum(n, place, 8, partial, ready, finish, rider, gather_rider, out_ref, gain_acc, bufs, sems)
    for j in (count - 2, count - 1):
        for copy in stores(j):
            copy.wait()
    for way in range(2):
        gsum_ref[core, way] = jnp.sum(gain_acc[0, way], axis=0, keepdims=True)
        gsum_ref[1 - core, way] = jnp.sum(gain_acc[1, way], axis=0, keepdims=True)


def final_kernel(*refs):
    half = len(refs) // 2
    for src, dst in zip(refs[:half], refs[half:]):
        dst[...] = src[...]


def final(out, gh, dw, dwo):
    seq, d = out.shape
    inner = dwo.shape[0]
    steps = seq // ROWS
    row = lambda a: pl.BlockSpec((a.shape[0] // steps, a.shape[1]), lambda j: (j, 0))
    part = lambda w, at: pl.BlockSpec((d // steps, w), lambda j: (j, at))
    shape = jax.ShapeDtypeStruct
    return pl.pallas_call(
        final_kernel, grid=(steps,),
        in_specs=[row(out), row(gh), part(inner, 0), part(HEAD_DIM, inner // HEAD_DIM), part(HEAD_DIM, inner // HEAD_DIM + 1), row(dwo)],
        out_specs=[row(out), row(gh), part(inner, 0), part(HEAD_DIM, 0), part(HEAD_DIM, 0), row(dwo)],
        out_shape=[shape(out.shape, BF16), shape(gh.shape, BF16), shape((d, inner), F32), shape((d, HEAD_DIM), F32),
                   shape((d, HEAD_DIM), F32), shape(dwo.shape, F32)],
        compiler_params=pltpu.CompilerParams(vmem_limit_bytes=VMEM_LIMIT),
        cost_estimate=pl.CostEstimate(flops=seq * d, bytes_accessed=12 * seq * d, transcendentals=0),
        name='final')(out, gh, dw, dw, dw, dwo)


def out_sum(n, wo, q, k, v, low, high, x, dout):
    seq, d_model = x.shape
    half, block, inner = d_model // 2, seq // n, q.shape[1]
    vmem, hbm = pl.BlockSpec(memory_space=pltpu.VMEM), pl.BlockSpec(memory_space=pl.ANY)
    shape = jax.ShapeDtypeStruct
    dma = pltpu.SemaphoreType.DMA
    rows32 = pltpu.VMEM((seq, inner), F32)
    wide32 = pltpu.VMEM((inner, half), F32)
    return pl.pallas_call(
        functools.partial(out_kernel, n),
        out_shape=[shape((seq, d_model), BF16), shape(q.shape, BF16), shape((seq, 2 * inner + 2 * HEAD_DIM), BF16)],
        in_specs=[vmem] * 6 + [hbm] * 2, out_specs=[hbm, vmem, vmem],
        scratch_shapes=[pltpu.VMEM((seq, 2 * inner), BF16), pltpu.VMEM((2 * inner, half), BF16),
                        pltpu.VMEM((block, half), BF16), pltpu.VMEM((2, ROWS, d_model), BF16), pltpu.VMEM((ROWS, inner), BF16),
                        pltpu.VMEM((seq, HEAD_DIM), F32), rows32, rows32, wide32, rows32, wide32, rows32, rows32,
                        dma((SUBS,)), dma((2,)), dma((3,)), dma((3,)), dma((SUBS,)), dma((SUBS,))]
        + ring_scratch(n, seq, d_model, 0),
        compiler_params=pltpu.CompilerParams(collective_id=1, has_side_effects=True, vmem_limit_bytes=VMEM_LIMIT),
        cost_estimate=pl.CostEstimate(flops=10 * seq * seq * HEAD_DIM, bytes_accessed=4 * seq * d_model, transcendentals=seq * seq),
        name='out_sum')(wo, q, k, v, low, high, x, dout)


def grad_sum(n, dlhs, o, wq_sib, gain, wq, wk, wv, x, dout, normed):
    seq, d_model = x.shape
    half, block, width = d_model // 2, seq // n, d_model // 4
    kdim, inner = dlhs.shape[1], o.shape[1]
    vmem, hbm = pl.BlockSpec(memory_space=pltpu.VMEM), pl.BlockSpec(memory_space=pl.ANY)
    shape = jax.ShapeDtypeStruct
    dma = pltpu.SemaphoreType.DMA
    return pl.pallas_call(
        functools.partial(grad_kernel, n),
        out_shape=[shape((seq, d_model), BF16), shape((2, 2, 1, width), F32), shape((d_model, 2 * inner), F32), shape((inner, d_model), F32)],
        in_specs=[vmem] * 4 + [hbm] * 6, out_specs=[hbm, vmem, hbm, hbm],
        scratch_shapes=[pltpu.VMEM((2, seq, ROWS), BF16), pltpu.VMEM((2, seq, ROWS), BF16),
                        pltpu.VMEM((2, ROWS, 2 * inner), F32), pltpu.VMEM((2, inner, ROWS), F32), dma((2, 2)), dma((2, 2)),
                        pltpu.VMEM((half, kdim), BF16), pltpu.VMEM((1, half), F32),
                        pltpu.VMEM((block, d_model), BF16), pltpu.VMEM((block, half), BF16), pltpu.VMEM((block, half), F32),
                        pltpu.VMEM((3, block, HEAD_DIM), F32), pltpu.VMEM((2, 2, 8, width), F32),
                        dma((3 + 2 * SUBS,)), dma((SUBS,)), dma((SUBS,))]
        + ring_scratch(n, seq, d_model, 8),
        compiler_params=pltpu.CompilerParams(collective_id=2, has_side_effects=True, vmem_limit_bytes=VMEM_LIMIT),
        cost_estimate=pl.CostEstimate(flops=4 * seq * kdim * half, bytes_accessed=4 * seq * d_model, transcendentals=0),
        name='grad_sum')(dlhs, o, wq_sib, gain, wq, wk, wv, x, dout, normed)


def solution(mesh):
    tp_size = mesh.shape['tp']
    chips = tp_size // 2
    swap = [(source, source ^ 1) for source in range(tp_size)]

    def block_fn(hidden, grad_out, norm_gain, w_query, w_key, w_value, w_out):
        batch, seq_len, d_model = hidden.shape
        half = d_model // 2
        tp_index = lax.axis_index('tp')
        kv_index, core = tp_index // 2, tp_index % 2
        low, high = rope_tables(seq_len // ROWS)
        x, dout = hidden[0], grad_out[0]
        gain = norm_gain[None, :]
        scalars = jnp.stack([kv_index, 1 - core])
        n, q, k, v, wq32 = front(scalars, x, gain, w_query, w_key, w_value, low, high)
        wq_sib = lax.ppermute(wq32, 'tp', swap)
        out, o, dlhs = out_sum(chips, w_out, q, k, v, low, high, x, dout)
        gh, gain_sum, dw, dwo = grad_sum(chips, dlhs, o, wq_sib, gain, w_query, w_key, w_value, x, dout, n)
        out, gh, grad_w_query, grad_w_key, grad_w_value, grad_w_out = final(out, gh, dw, dwo)
        return out[None], gh[None], gain_sum.reshape(-1), grad_w_query, grad_w_key, grad_w_value, grad_w_out

    act_spec = P('dp', None, None)
    return jax.shard_map(
        block_fn, mesh=mesh,
        in_specs=(act_spec, act_spec, P(None), P(None, 'tp'), P(None, None), P(None, None), P('tp', None)),
        out_specs=(act_spec, act_spec, P('dp'), P('dp', 'tp'), P('dp', 'tp'), P('dp', 'tp'), P(('dp', 'tp'), None)),
        check_vma=False)
```

```python
import functools
import math
import jax
import jax.numpy as jnp
import numpy as np
from jax import lax
from jax.experimental import pallas as pl
from jax.experimental.pallas import tpu as pltpu
from jax.sharding import PartitionSpec as P

HEAD_DIM = 128
NORM_EPS = 1.0e-5
ROPE_BASE = 10000.0
MASK_VALUE = -1.0e30
SCORE_SCALE = 1.0 / math.sqrt(HEAD_DIM)
EXP2_SCALE = SCORE_SCALE * math.log2(math.e)
ROWS = 256
WIDE = 512
BF16 = jnp.bfloat16
F32 = jnp.float32
VMEM_LIMIT = 66 * 10**6


def dot(a, b, contract):
    return lax.dot_general(a, b, ((contract[:1], contract[1:]), ((), ())), preferred_element_type=F32)


def rope_tables(count):
    def table(positions):
        inv_freq = ROPE_BASE ** (-np.arange(0, HEAD_DIM, 2, dtype=np.float64) / HEAD_DIM)
        angles = positions[:, None] * inv_freq[None, :]
        cos_t = np.repeat(np.cos(angles), 2, axis=1)
        sin_t = np.stack([-np.sin(angles), np.sin(angles)], axis=-1).reshape(cos_t.shape)
        return np.stack([cos_t, sin_t]).astype(np.float32)
    return table(np.arange(ROWS, dtype=np.float64)), table(ROWS * np.arange(count, dtype=np.float64))


def rope_block(b, low_ref, high_ref):
    cos_b, sin_b = high_ref[0, pl.ds(b, 1), :], high_ref[1, pl.ds(b, 1), :]
    cos_l, sin_l = low_ref[0], low_ref[1]
    return cos_b * cos_l - sin_b * sin_l, sin_b * cos_l + cos_b * sin_l


def rotate(t, cos_t, sin_t):
    even = lax.broadcasted_iota(jnp.int32, t.shape, 1) % 2 == 0
    swapped = jnp.where(even, pltpu.roll(t, HEAD_DIM - 1, 1), pltpu.roll(t, 1, 1))
    return t * cos_t + swapped * sin_t


def front_kernel(kv_ref, x_ref, gain_ref, wq_ref, wk_ref, wv_ref, low_ref, high_ref,
                 n_ref, q_ref, k_ref, v_ref, wq32_ref, gain_row, wqkv):
    i = pl.program_id(0)
    half = wq32_ref.shape[0]
    gain = gain_ref[...].astype(F32).reshape(gain_row.shape)

    @pl.when(i == 0)
    def _():
        wqkv[:, :2 * HEAD_DIM] = wq_ref[...]
        wqkv[:, 2 * HEAD_DIM:3 * HEAD_DIM] = wk_ref[...]
        wqkv[:, 3 * HEAD_DIM:] = wv_ref[...]
        gain_row[...] = gain
        wq32_ref[...] = wq_ref[pl.ds(pl.multiple_of(kv_ref[1] * half, half), half), :].astype(F32)

    parts = []
    for r in range(0, WIDE, ROWS):
        rows = slice(r, r + ROWS)
        x = x_ref[rows, :].astype(F32)
        inv = lax.rsqrt(jnp.mean(x * x, axis=-1, keepdims=True) + NORM_EPS)
        n_ref[rows, :] = (x * inv * gain).astype(BF16)
        parts.append(rope_block(i * (WIDE // ROWS) + r // ROWS, low_ref, high_ref))
    qkv = dot(n_ref[...], wqkv[...], (1, 0))
    cos_t, sin_t = (jnp.concatenate([p[t] for p in parts], axis=0) for t in range(2))
    q0 = rotate(qkv[:, :HEAD_DIM], cos_t, sin_t).astype(BF16)
    q1 = rotate(qkv[:, HEAD_DIM:2 * HEAD_DIM], cos_t, sin_t).astype(BF16)
    k = rotate(qkv[:, 2 * HEAD_DIM:3 * HEAD_DIM], cos_t, sin_t).astype(BF16)
    v = qkv[:, 3 * HEAD_DIM:].astype(BF16)
    q_ref[:, :HEAD_DIM] = q0
    q_ref[:, HEAD_DIM:] = q1
    k_ref[...] = k
    v_ref[...] = v


def front(scalars, x, gain, wq, wk, wv, low, high):
    seq, d = x.shape
    row = lambda w: pl.BlockSpec((WIDE, w), lambda i, kv: (i, 0))
    whole = lambda shape: pl.BlockSpec(shape, lambda i, kv: (0,) * len(shape))
    head = pl.BlockSpec((d, HEAD_DIM), lambda i, kv: (0, kv[0]))
    widths = (d, 2 * HEAD_DIM, HEAD_DIM, HEAD_DIM)
    return pl.pallas_call(
        front_kernel,
        grid_spec=pltpu.PrefetchScalarGridSpec(
            num_scalar_prefetch=1, grid=(seq // WIDE,),
            in_specs=[row(d), whole(gain.shape), whole(wq.shape), head, head, whole(low.shape), whole(high.shape)],
            out_specs=[row(w) for w in widths] + [whole((d // 2, wq.shape[1])), whole((1, d))],
            scratch_shapes=[pltpu.VMEM((d, 4 * HEAD_DIM), BF16)]),
        out_shape=[jax.ShapeDtypeStruct((seq, w), BF16) for w in widths] + [jax.ShapeDtypeStruct((d // 2, wq.shape[1]), F32), jax.ShapeDtypeStruct((1, d), F32)],
        compiler_params=pltpu.CompilerParams(vmem_limit_bytes=VMEM_LIMIT),
        cost_estimate=pl.CostEstimate(flops=2 * seq * d * 4 * HEAD_DIM, bytes_accessed=5 * seq * d, transcendentals=0),
        name='front')(scalars, x, gain, wq, wk, wv, low, high)


def attn_fwd_rows(c, q_ref, k_ref, v_ref, o_ref):
    lo, hi = c * WIDE, (c + 1) * WIDE

    def block(r, carry):
        rows = pl.ds(pl.multiple_of(lo + r * ROWS, ROWS), ROWS)
        q2 = jnp.concatenate([q_ref[rows, :HEAD_DIM], q_ref[rows, HEAD_DIM:]], axis=0)
        row_id = lax.broadcasted_iota(jnp.int32, (2 * ROWS, WIDE), 0) % ROWS + r * ROWS
        causal = row_id >= lax.broadcasted_iota(jnp.int32, (2 * ROWS, WIDE), 1)
        s_diag = jnp.where(causal, dot(q2, k_ref[lo:hi, :], (1, 1)), MASK_VALUE)
        m = jnp.max(s_diag, axis=-1, keepdims=True)
        if lo:
            s_pre = dot(q2, k_ref[:lo, :], (1, 1))
            m = jnp.maximum(m, jnp.max(s_pre, axis=-1, keepdims=True))
        p_diag = jnp.exp2((s_diag - m) * EXP2_SCALE)
        total = jnp.sum(p_diag, axis=-1, keepdims=True)
        if lo:
            p_pre = jnp.exp2((s_pre - m) * EXP2_SCALE)
            total = total + jnp.sum(p_pre, axis=-1, keepdims=True)
        scale = 1.0 / total
        o2 = dot((p_diag * scale).astype(BF16), v_ref[lo:hi, :], (1, 0))
        if lo:
            o2 = o2 + dot((p_pre * scale).astype(BF16), v_ref[:lo, :], (1, 0))
        o_ref[rows, :HEAD_DIM] = o2[:ROWS].astype(BF16)
        o_ref[rows, HEAD_DIM:] = o2[ROWS:].astype(BF16)
        return carry

    lax.fori_loop(0, WIDE // ROWS, block, 0)


def attn_bwd_rows(i, head, c, do_both, q_ref, k_ref, v_ref, low_ref, high_ref, dq32, dk_acc, dv_acc):
    lo, hi = c * WIDE, (c + 1) * WIDE
    rows = pl.ds(pl.multiple_of(i * ROWS, ROWS), ROWS)
    query_id = lax.broadcasted_iota(jnp.int32, (WIDE, ROWS), 1) + (i * ROWS - lo)
    causal = lax.broadcasted_iota(jnp.int32, (WIDE, ROWS), 0) <= query_id

    cols = pl.ds(pl.multiple_of(head * HEAD_DIM, HEAD_DIM), HEAD_DIM)
    q, do = q_ref[rows, cols], do_both[:, cols]
    k_all, v_all = k_ref[:hi, :], v_ref[:hi, :]
    s_t = dot(k_all, q, (1, 1))
    s_diag = jnp.where(causal, s_t[lo:], MASK_VALUE)
    s_t = jnp.concatenate([s_t[:lo], s_diag], axis=0) if lo else s_diag
    m = jnp.max(s_t, axis=0, keepdims=True)
    p = jnp.exp2((s_t - m) * EXP2_SCALE)
    p = p * (1.0 / jnp.sum(p, axis=0, keepdims=True))
    dp = dot(v_all, do, (1, 1))
    delta = jnp.sum(p * dp, axis=0, keepdims=True)
    ds = (p * (dp - delta) * SCORE_SCALE).astype(BF16)
    dv_acc[:hi, :] += dot(p.astype(BF16), do, (1, 0))
    dk_acc[:hi, :] += dot(ds, q, (1, 0))
    dq = dot(ds, k_all, (0, 0))
    cos_t, sin_t = rope_block(i, low_ref, high_ref)
    dq32[rows, cols] = rotate(dq, cos_t, -sin_t).astype(BF16).astype(F32)


SUBS = 4


def ring_kernel_setup(n):
    me = lax.axis_index('tp')
    chip, core = me // 2, me % 2
    right = (chip + 1) % n * 2 + core
    left = (chip + n - 1) % n * 2 + core
    sib = me + 1 - 2 * core
    barrier = pltpu.get_barrier_semaphore()
    for peer in (right, left, sib):
        pl.semaphore_signal(barrier, inc=1, device_id={'tp': peer}, device_id_type=pl.DeviceIdType.MESH)
    return chip, core, right, left, sib


def peers_ready():
    pl.semaphore_wait(pltpu.get_barrier_semaphore(), 3)


def remote(src, dst, send, recv, peer):
    return pltpu.make_async_remote_copy(src_ref=src, dst_ref=dst, send_sem=send, recv_sem=recv,
                                        device_id={'tp': peer}, device_id_type=pl.DeviceIdType.MESH)


def owned_rows(n, sub_rows, chip, sub):
    return pl.ds(pl.multiple_of((sub * n + chip) * sub_rows, sub_rows), sub_rows)


def ring_sum(n, place, extra, partial, ready, finish, rider, gather_rider, out_ref, gain_acc, bufs, sems):
    chip, core, right, left, sib = place
    rs_buf, ag_buf, sib_buf, obuf = bufs
    rs_send, rs_recv, ag_send, ag_recv, sib_send, sib_recv, out_sem, credit = sems
    width = rs_buf.shape[-1]
    block = out_ref.shape[0] // n
    sub_rows = block // SUBS
    half = 2 * width
    peers = (right, left)

    def local(sub):
        start = sub * sub_rows
        return pl.ds(start if isinstance(sub, int) else pl.multiple_of(start, sub_rows), sub_rows)

    def part(slot_ref, sub, with_extra):
        if with_extra:
            return slot_ref.at[pl.ds(sub * sub_rows, sub_rows + (extra if sub == SUBS - 1 else 0)), :]
        return slot_ref.at[local(sub), :]

    def rs_copy(s, sub, way):
        return remote(part(rs_buf.at[way, s], sub, False), part(rs_buf.at[way, s + 1], sub, False),
                      rs_send.at[way, s, sub], rs_recv.at[way, s, sub], peers[way])

    def ag_copy(s, sub, way):
        return remote(part(ag_buf.at[way, s], sub, True), part(ag_buf.at[way, s + 1], sub, True),
                      ag_send.at[way, s, sub], ag_recv.at[way, s, sub], peers[way])

    def sib_copy(s, sub, way):
        rows = sub_rows + (extra if sub == SUBS - 1 else 0)
        k = SUBS * s + sub
        return remote(part(ag_buf.at[way, s], sub, True), sib_buf.at[way, k % (2 * SUBS), pl.ds(0, rows), :],
                      sib_send.at[way, k], sib_recv.at[way, k], sib)

    def my_part(dest, sub, way):
        return partial(owned_rows(n, sub_rows, dest, sub), way)

    def dest_of(s, way):
        return (chip + n - 1 - s) % n if way == 0 else (chip + 1 + s) % n

    for sub in range(SUBS):
        ready(sub)
        for way in range(2):
            rs_buf[way, 0, local(sub), :] = my_part(dest_of(0, way), sub, way)
            rs_copy(0, sub, way).start()

    def rs_step(k, carry):
        s, sub = k // SUBS, k % SUBS
        for way in range(2):
            term = my_part(dest_of(s, way), sub, way)
            rs_copy(s - 1, sub, way).wait_recv()
            rs_buf[way, s, local(sub), :] += term
            rs_copy(s, sub, way).start()
        rider(s, sub)
        return carry

    lax.fori_loop(SUBS, SUBS * (n - 1), rs_step, 0)

    def out_copy(whose, s, sub, way):
        b = (chip + n - s) % n if way == 0 else (chip + s) % n
        col = (core if whose == 0 else 1 - core) * half + way * width
        dst = out_ref.at[owned_rows(n, sub_rows, b, sub), pl.ds(pl.multiple_of(col, 128), width)]
        return pltpu.make_async_copy(obuf.at[whose, sub, way], dst, out_sem.at[whose, sub, way])

    def emit(whose, s, sub, way, values):
        @pl.when(s >= 1)
        def _():
            out_copy(whose, s - 1, sub, way).wait()
        obuf[whose, sub, way] = values.astype(BF16)
        out_copy(whose, s, sub, way).start()

    def own_chunk(s, sub, forward):
        @pl.when(s >= 2)
        def _():
            pl.semaphore_wait(credit, 1)
        for way in range(2):
            if forward:
                ag_copy(s, sub, way).start()
            sib_copy(s, sub, way).start()
        for way in range(2):
            emit(0, s, sub, way, ag_buf[way, s, local(sub), :])
            if extra and sub == SUBS - 1:
                gain_acc[0, way] += ag_buf[way, s, pl.ds(block, extra), :]

    def sib_chunk(s, sub):
        k = SUBS * s + sub
        for way in range(2):
            sib_copy(s, sub, way).wait_recv()
            emit(1, s, sub, way, sib_buf[way, k % (2 * SUBS), pl.ds(0, sub_rows), :])
            if extra and sub == SUBS - 1:
                gain_acc[1, way] += sib_buf[way, k % (2 * SUBS), pl.ds(sub_rows, extra), :]

        @pl.when(s < n - 2)
        def _():
            pl.semaphore_signal(credit, inc=1, device_id={'tp': sib}, device_id_type=pl.DeviceIdType.MESH)

    for sub in range(SUBS):
        terms = [my_part(chip, sub, way) for way in range(2)]
        for way in range(2):
            rs_copy(n - 2, sub, way).wait_recv()
        finish(sub, [rs_buf[way, n - 1, local(sub), :] + terms[way] for way in range(2)])
        own_chunk(0, sub, True)
        if sub:
            sib_chunk(0, sub - 1)

    def ag_step(s, carry):
        for sub in range(SUBS):
            for way in range(2):
                ag_copy(s - 1, sub, way).wait_recv()
            own_chunk(s, sub, True)
            if sub == 0:
                sib_chunk(s - 1, SUBS - 1)
                gather_rider(s)
            else:
                sib_chunk(s, sub - 1)
        return carry

    lax.fori_loop(1, n - 1, ag_step, 0)
    last = n - 1
    for sub in range(SUBS):
        for way in range(2):
            ag_copy(last - 1, sub, way).wait_recv()
        own_chunk(last, sub, False)
        if sub == 0:
            sib_chunk(last - 1, SUBS - 1)
        else:
            sib_chunk(last, sub - 1)
    sib_chunk(last, SUBS - 1)
    for sub in range(SUBS):
        for way in range(2):
            for whose in range(2):
                out_copy(whose, last, sub, way).wait()

    def drain(s, carry):
        for sub in range(SUBS):
            for way in range(2):
                rs_copy(s, sub, way).wait_send()
                ag_copy(s, sub, way).wait_send()
                sib_copy(s, sub, way).wait_send()
        return carry

    lax.fori_loop(0, n - 1, drain, 0)
    for sub in range(SUBS):
        for way in range(2):
            sib_copy(last, sub, way).wait_send()


def ring_scratch(n, seq, d_model, extra):
    width, block = d_model // 4, seq // n
    sub_rows = block // SUBS
    dma = pltpu.SemaphoreType.DMA
    return [
        pltpu.VMEM((2, n, block, width), F32),
        pltpu.VMEM((2, n, block + extra, width), F32),
        pltpu.VMEM((2, 2 * SUBS, sub_rows + extra, width), F32),
        pltpu.VMEM((2, SUBS, 2, sub_rows, width), BF16),
        dma((2, n - 1, SUBS)), dma((2, n - 1, SUBS)), dma((2, n - 1, SUBS)), dma((2, n - 1, SUBS)),
        dma((2, SUBS * n)), dma((2, SUBS * n)), dma((2, SUBS, 2)), pltpu.SemaphoreType.REGULAR,
    ]


def out_kernel(n, wo_ref, q_ref, k_ref, v_ref, low_ref, high_ref, x_ref, dout_ref,
               out_ref, o_ref, dlhs_ref, lhs, rhs, x_rows, dout_rows, do_blk, dk_acc, x32, dkv32, wo32, o_got, wo_got, dq_got, dkv_got,
               row_sem, dout_sem, swap_send, swap_recv, o_send, o_recv, *ring):
    bufs, sems = ring[:4], ring[4:]
    place = ring_kernel_setup(n)
    chip, core, right, left, sib = place
    width = bufs[0].shape[-1]
    half = 2 * width
    block = x_rows.shape[0]
    sub_rows = block // SUBS
    inner = o_ref.shape[1]
    wide = n * sub_rows
    my_cols = pl.ds(pl.multiple_of(core * half, 128), half)

    def x_copy(sub):
        return pltpu.make_async_copy(x_ref.at[owned_rows(n, sub_rows, chip, sub), my_cols],
                                     x_rows.at[pl.ds(sub * sub_rows, sub_rows), :], row_sem.at[sub])

    def dout_copy(i):
        return pltpu.make_async_copy(dout_ref.at[pl.ds(pl.multiple_of(i * ROWS, ROWS), ROWS), :], dout_rows.at[i % 2], dout_sem.at[i % 2])

    swaps = [remote(src, dst, swap_send.at[k], swap_recv.at[k], sib)
             for k, (src, dst) in enumerate([(wo32, wo_got), (x32, dq_got), (dkv32, dkv_got)])]

    def o_swap(w):
        rows = pl.ds(w * wide, wide)
        return remote(x32.at[rows, :], o_got.at[rows, :], o_send.at[w], o_recv.at[w], sib)

    def forward(w):
        rows = pl.ds(w * wide, wide)
        attn_fwd_rows(w, q_ref, k_ref, v_ref, o_ref)
        x32[rows, :] = o_ref[rows, :].astype(F32)
        o_swap(w).start()
        lhs[rows, :inner] = o_ref[rows, :]

    for sub in range(SUBS):
        x_copy(sub).start()
    dout_copy(0).start()
    wo32[...] = wo_ref[:, pl.ds(pl.multiple_of((1 - core) * half, 128), half)].astype(F32)
    peers_ready()
    swaps[0].start()
    forward(0)
    rhs[:inner, :] = wo_ref[:, my_cols]
    swaps[0].wait()
    rhs[inner:, :] = wo_got[...].astype(BF16)

    def ready(sub):
        if sub + 1 < SUBS:
            forward(sub + 1)
        o_swap(sub).wait()
        rows = pl.ds(sub * wide, wide)
        lhs[rows, inner:] = o_got[rows, :].astype(BF16)
        if sub == SUBS - 1:
            dk_acc[...] = jnp.zeros_like(dk_acc)
            dkv32[:, HEAD_DIM:] = jnp.zeros_like(dk_acc)

    def partial(rows, way):
        return dot(lhs[rows, :], rhs[:, way * width:(way + 1) * width], (1, 0))

    def finish(sub, sums):
        x_copy(sub).wait()
        for way in range(2):
            rows = pl.ds(sub * sub_rows, sub_rows)
            bufs[1][way, 0, rows, :] = sums[way] + x_rows[rows, way * width:(way + 1) * width].astype(F32)

    dv_acc = dkv32.at[:, pl.ds(HEAD_DIM, HEAD_DIM)]
    count = q_ref.shape[0] // ROWS
    per_wide = WIDE // ROWS

    def ride(i, head, wides):
        @pl.when(head == 0)
        def _():
            dout_copy(i).wait()
            pl.when(i + 1 < count)(lambda: dout_copy(i + 1).start())
            do_blk[...] = dot(dout_rows[i % 2], wo_ref[...], (1, 1)).astype(BF16)
        for c in wides:
            pl.when(i // per_wide == c)(
                lambda c=c: attn_bwd_rows(i, head, c, do_blk, q_ref, k_ref, v_ref, low_ref, high_ref, x32, dk_acc, dv_acc))

    early = n - 2

    def rider(step, sub):
        pl.when(sub % 2 == 0)(lambda: ride(step - 1, sub // 2, range((early - 1) // per_wide + 1)))

    def gather_rider(step):
        @pl.when(step <= 2 * (count - early))
        def _():
            ride(early + (step - 1) // 2, (step - 1) % 2, range(early // per_wide, count // per_wide))

        @pl.when(step == 2 * (count - early) + 1)
        def _():
            def turn_back(b, carry):
                rows = pl.ds(pl.multiple_of(b * ROWS, ROWS), ROWS)
                cos_t, sin_t = rope_block(b, low_ref, high_ref)
                dkv32[rows, :HEAD_DIM] = rotate(dk_acc[rows, :], cos_t, -sin_t)
                return carry
            lax.fori_loop(0, count, turn_back, 0)
            swaps[1].start()
            swaps[2].start()

        @pl.when(step == n - 2)
        def _():
            swaps[1].wait()
            swaps[2].wait()
            dlhs_ref[:, :inner] = x32[...].astype(BF16)
            dlhs_ref[:, inner:2 * inner] = (dkv32[...] + dkv_got[...]).astype(BF16)
            dlhs_ref[:, 2 * inner:] = dq_got[...].astype(BF16)

    ring_sum(n, place, 0, partial, ready, finish, rider, gather_rider, out_ref, None, bufs, sems)


def grad_kernel(n, lhs, o_ref, wqsib_ref, gain_ref, wq_ref, wk_ref, wv_ref, x_ref, dout_ref, n_ref,
                out_ref, gsum_ref, dw_ref, dwo_ref, n_blk, dout_blk, dw_blk, dwo_blk, blk_sem, dw_sem, rhs, gain, x_rows, dout_rows, unit_buf, stat_buf, gain_acc, row_sem, stat_send, stat_recv, *ring):
    bufs, sems = ring[:4], ring[4:]
    place = ring_kernel_setup(n)
    chip, core, right, left, sib = place
    width = bufs[0].shape[-1]
    block = x_rows.shape[0]
    inner = wq_ref.shape[1]
    half = 2 * width
    col = pl.multiple_of(core * half, 128)
    head_cols = pl.ds(pl.multiple_of(chip * HEAD_DIM, HEAD_DIM), HEAD_DIM)
    sub_rows = block // SUBS
    rows_copies = []
    for sub in range(SUBS):
        src, dst = owned_rows(n, sub_rows, chip, sub), pl.ds(sub * sub_rows, sub_rows)
        rows_copies += [pltpu.make_async_copy(x_ref.at[src, :], x_rows.at[dst, :], row_sem.at[3 + 2 * sub]),
                        pltpu.make_async_copy(dout_ref.at[src, pl.ds(col, half)], dout_rows.at[dst, :], row_sem.at[4 + 2 * sub])]
    weights = [
        pltpu.make_async_copy(wq_ref.at[pl.ds(col, half), :], rhs.at[:, pl.ds(0, inner)], row_sem.at[0]),
        pltpu.make_async_copy(wk_ref.at[pl.ds(col, half), head_cols], rhs.at[:, pl.ds(inner, HEAD_DIM)], row_sem.at[1]),
        pltpu.make_async_copy(wv_ref.at[pl.ds(col, half), head_cols], rhs.at[:, pl.ds(inner + HEAD_DIM, HEAD_DIM)], row_sem.at[2]),
    ]
    count = n_ref.shape[1] // ROWS

    def loads(j):
        cols = pl.ds(pl.multiple_of(j * ROWS, ROWS), ROWS)
        return [pltpu.make_async_copy(n_ref.at[:, cols], n_blk.at[j % 2], blk_sem.at[0, j % 2]),
                pltpu.make_async_copy(dout_ref.at[:, cols], dout_blk.at[j % 2], blk_sem.at[1, j % 2])]

    def stores(j):
        cols = pl.ds(pl.multiple_of(j * ROWS, ROWS), ROWS)
        return [pltpu.make_async_copy(dw_blk.at[j % 2], dw_ref.at[cols, :], dw_sem.at[0, j % 2]),
                pltpu.make_async_copy(dwo_blk.at[j % 2], dwo_ref.at[:, cols], dw_sem.at[1, j % 2])]

    def weight_block(j):
        for copy in loads(j):
            copy.wait()

        @pl.when(j + 1 < count)
        def _():
            for copy in loads(j + 1):
                copy.start()

        @pl.when(j >= 2)
        def _():
            for copy in stores(j - 2):
                copy.wait()
        dw_blk[j % 2] = dot(n_blk[j % 2], lhs[:, :2 * inner], (0, 0))
        dwo_blk[j % 2] = dot(o_ref[...], dout_blk[j % 2], (0, 0))
        for copy in stores(j):
            copy.start()

    for copy in weights + rows_copies + loads(0):
        copy.start()
    rhs[:, inner + 2 * HEAD_DIM:] = wqsib_ref[...].astype(BF16)
    gain[...] = gain_ref[:, pl.ds(col, half)]
    for copy in weights:
        copy.wait()
    peers_ready()
    gain_acc[...] = jnp.zeros_like(gain_acc)

    def partial(rows, way):
        return dot(lhs[rows, :], rhs[way * width:(way + 1) * width, :], (1, 1))

    def prepare(sub):
        rows = pl.ds(sub * sub_rows, sub_rows)
        x = x_rows[rows, :].astype(F32)
        inv = lax.rsqrt(jnp.mean(x * x, axis=-1, keepdims=True) + NORM_EPS)
        stat_buf[2, rows, :] = jnp.broadcast_to(inv, (sub_rows, HEAD_DIM))
        mine = x_rows[rows, pl.ds(col, half)].astype(F32)
        unit_buf[rows, :] = mine * inv

    def ready(sub):
        if sub == SUBS - 1:
            for copy in rows_copies:
                copy.wait()

    def rider(step, sub):
        @pl.when((step == 1) & (sub == 0))
        def _():
            for own in range(SUBS):
                prepare(own)
        pl.when((sub == 1) & (step - 1 < count))(lambda: weight_block(step - 1))

    def gather_rider(step):
        pl.when(step + n - 3 < count)(lambda: weight_block(step + n - 3))

    def stat_copy(sub):
        rows = pl.ds(sub * sub_rows, sub_rows)
        return remote(stat_buf.at[0, rows, :], stat_buf.at[1, rows, :], stat_send.at[sub], stat_recv.at[sub], sib)

    def finish(sub, sums):
        rows = pl.ds(sub * sub_rows, sub_rows)
        ag_buf = bufs[1]
        total = jnp.zeros((sub_rows, 1), F32)
        for way in range(2):
            cols = slice(way * width, (way + 1) * width)
            unit = unit_buf[rows, cols]
            prod = sums[way] * unit
            total = total + jnp.sum(prod * gain[:, cols], axis=-1, keepdims=True)
            gsum = jnp.sum(prod.reshape(sub_rows // 8, 8, width), axis=0)
            ag_buf[way, 0, pl.ds(block, 8), :] = gsum if sub == 0 else gsum + ag_buf[way, 0, pl.ds(block, 8), :]
            ag_buf[way, 0, rows, :] = sums[way]
        stat_buf[0, rows, :] = jnp.broadcast_to(total, (sub_rows, HEAD_DIM))
        stat_copy(sub).start()
        stat_copy(sub).wait()
        mean = (stat_buf[0, rows, 0:1] + stat_buf[1, rows, 0:1]) * (1.0 / (2 * half))
        inv = stat_buf[2, rows, 0:1]
        for way in range(2):
            cols = slice(way * width, (way + 1) * width)
            scaled = ag_buf[way, 0, rows, :] * gain[:, cols]
            ag_buf[way, 0, rows, :] = dout_rows[rows, cols].astype(F32) + inv * (scaled - unit_buf[rows, cols] * mean)

    ring_sum(n, place, 8, partial, ready, finish, rider, gather_rider, out_ref, gain_acc, bufs, sems)
    for j in (count - 2, count - 1):
        for copy in stores(j):
            copy.wait()
    for way in range(2):
        for whose, start in ((0, col), (1, (1 - core) * half)):
            cols = pl.ds(pl.multiple_of(start + way * width, 128), width)
            gsum_ref[:, cols] = jnp.sum(gain_acc[whose, way], axis=0, keepdims=True)


def final_kernel(*refs):
    half = len(refs) // 2
    for src, dst in zip(refs[:half], refs[half:]):
        dst[...] = src[...].reshape(dst.shape)


def final(out, gh, dw, dwo, gain_sum):
    seq, d = out.shape
    inner = dwo.shape[0]
    steps = seq // WIDE
    row = lambda a: pl.BlockSpec((a.shape[0] // steps, a.shape[1]), lambda j: (j, 0))
    part = lambda w, at: pl.BlockSpec((d // steps, w), lambda j: (j, at))
    shape = jax.ShapeDtypeStruct
    return pl.pallas_call(
        final_kernel, grid=(steps,),
        in_specs=[row(out), row(gh), part(inner, 0), part(HEAD_DIM, inner // HEAD_DIM), part(HEAD_DIM, inner // HEAD_DIM + 1), row(dwo),
                  pl.BlockSpec((1, d), lambda j: (0, 0))],
        out_specs=[row(out), row(gh), part(inner, 0), part(HEAD_DIM, 0), part(HEAD_DIM, 0), row(dwo), pl.BlockSpec((d,), lambda j: (0,))],
        out_shape=[shape(out.shape, BF16), shape(gh.shape, BF16), shape((d, inner), F32), shape((d, HEAD_DIM), F32),
                   shape((d, HEAD_DIM), F32), shape(dwo.shape, F32), shape((d,), F32)],
        compiler_params=pltpu.CompilerParams(vmem_limit_bytes=VMEM_LIMIT),
        cost_estimate=pl.CostEstimate(flops=seq * d, bytes_accessed=12 * seq * d, transcendentals=0),
        name='final')(out, gh, dw, dw, dw, dwo, gain_sum)


def out_sum(n, wo, q, k, v, low, high, x, dout):
    seq, d_model = x.shape
    half, block, inner = d_model // 2, seq // n, q.shape[1]
    vmem, hbm = pl.BlockSpec(memory_space=pltpu.VMEM), pl.BlockSpec(memory_space=pl.ANY)
    shape = jax.ShapeDtypeStruct
    dma = pltpu.SemaphoreType.DMA
    rows32 = pltpu.VMEM((seq, inner), F32)
    wide32 = pltpu.VMEM((inner, half), F32)
    return pl.pallas_call(
        functools.partial(out_kernel, n),
        out_shape=[shape((seq, d_model), BF16), shape(q.shape, BF16), shape((seq, 2 * inner + 2 * HEAD_DIM), BF16)],
        in_specs=[vmem] * 6 + [hbm] * 2, out_specs=[hbm, vmem, vmem],
        scratch_shapes=[pltpu.VMEM((seq, 2 * inner), BF16), pltpu.VMEM((2 * inner, half), BF16),
                        pltpu.VMEM((block, half), BF16), pltpu.VMEM((2, ROWS, d_model), BF16), pltpu.VMEM((ROWS, inner), BF16),
                        pltpu.VMEM((seq, HEAD_DIM), F32), rows32, rows32, wide32, rows32, wide32, rows32, rows32,
                        dma((SUBS,)), dma((2,)), dma((3,)), dma((3,)), dma((SUBS,)), dma((SUBS,))]
        + ring_scratch(n, seq, d_model, 0),
        compiler_params=pltpu.CompilerParams(collective_id=1, has_side_effects=True, vmem_limit_bytes=VMEM_LIMIT),
        cost_estimate=pl.CostEstimate(flops=10 * seq * seq * HEAD_DIM, bytes_accessed=4 * seq * d_model, transcendentals=seq * seq),
        name='out_sum')(wo, q, k, v, low, high, x, dout)


def grad_sum(n, dlhs, o, wq_sib, gain, wq, wk, wv, x, dout, normed):
    seq, d_model = x.shape
    half, block, width = d_model // 2, seq // n, d_model // 4
    kdim, inner = dlhs.shape[1], o.shape[1]
    vmem, hbm = pl.BlockSpec(memory_space=pltpu.VMEM), pl.BlockSpec(memory_space=pl.ANY)
    shape = jax.ShapeDtypeStruct
    dma = pltpu.SemaphoreType.DMA
    return pl.pallas_call(
        functools.partial(grad_kernel, n),
        out_shape=[shape((seq, d_model), BF16), shape((1, d_model), F32), shape((d_model, 2 * inner), F32), shape((inner, d_model), F32)],
        in_specs=[vmem] * 4 + [hbm] * 6, out_specs=[hbm, vmem, hbm, hbm],
        scratch_shapes=[pltpu.VMEM((2, seq, ROWS), BF16), pltpu.VMEM((2, seq, ROWS), BF16),
                        pltpu.VMEM((2, ROWS, 2 * inner), F32), pltpu.VMEM((2, inner, ROWS), F32), dma((2, 2)), dma((2, 2)),
                        pltpu.VMEM((half, kdim), BF16), pltpu.VMEM((1, half), F32),
                        pltpu.VMEM((block, d_model), BF16), pltpu.VMEM((block, half), BF16), pltpu.VMEM((block, half), F32),
                        pltpu.VMEM((3, block, HEAD_DIM), F32), pltpu.VMEM((2, 2, 8, width), F32),
                        dma((3 + 2 * SUBS,)), dma((SUBS,)), dma((SUBS,))]
        + ring_scratch(n, seq, d_model, 8),
        compiler_params=pltpu.CompilerParams(collective_id=2, has_side_effects=True, vmem_limit_bytes=VMEM_LIMIT),
        cost_estimate=pl.CostEstimate(flops=4 * seq * kdim * half, bytes_accessed=4 * seq * d_model, transcendentals=0),
        name='grad_sum')(dlhs, o, wq_sib, gain, wq, wk, wv, x, dout, normed)


def solution(mesh):
    tp_size = mesh.shape['tp']
    chips = tp_size // 2
    swap = [(source, source ^ 1) for source in range(tp_size)]

    def block_fn(hidden, grad_out, norm_gain, w_query, w_key, w_value, w_out):
        batch, seq_len, d_model = hidden.shape
        half = d_model // 2
        tp_index = lax.axis_index('tp')
        kv_index, core = tp_index // 2, tp_index % 2
        low, high = rope_tables(seq_len // ROWS)
        x, dout = hidden[0], grad_out[0]
        scalars = jnp.stack([kv_index, 1 - core])
        n, q, k, v, wq32, gain = front(scalars, x, norm_gain, w_query, w_key, w_value, low, high)
        wq_sib = lax.ppermute(wq32, 'tp', swap)
        out, o, dlhs = out_sum(chips, w_out, q, k, v, low, high, x, dout)
        gh, gain_sum, dw, dwo = grad_sum(chips, dlhs, o, wq_sib, gain, w_query, w_key, w_value, x, dout, n)
        out, gh, grad_w_query, grad_w_key, grad_w_value, grad_w_out, grad_gain = final(out, gh, dw, dwo, gain_sum)
        return out[None], gh[None], grad_gain, grad_w_query, grad_w_key, grad_w_value, grad_w_out

    act_spec = P('dp', None, None)
    return jax.shard_map(
        block_fn, mesh=mesh,
        in_specs=(act_spec, act_spec, P(None), P(None, 'tp'), P(None, None), P(None, None), P('tp', None)),
        out_specs=(act_spec, act_spec, P('dp'), P('dp', 'tp'), P('dp', 'tp'), P('dp', 'tp'), P(('dp', 'tp'), None)),
        check_vma=False)
```
